32 devices in a mesh: groups: 2 (over y), ep: 4 (over z), sub: 4 (over x, core).
Axes of the slice: x: 2, y: 2, z: 4, core: 2. Of those that a mesh axis runs over, the one named last changes fastest.
Arguments:
- tokens: bfloat16 [512, 7168], P(('groups', 'ep'), 'sub'), parts along dimension 0, may hold values from -6 to 6
- expert_ids: int32 [512, 2], P(('groups', 'ep')), parts along dimension 0, may hold values from 0 to 3, all different within a row; in each aligned block of 64 rows (0 to 63, 64 to 127, ...) at most 48 rows name the same one
- route_weights: float32 [512, 2], P(('groups', 'ep')), parts along dimension 0, may hold values from 0.05 to 0.6
- gate_weight: bfloat16 [4, 7168, 1024], P('ep', 'sub'), may hold values from -0.0625 to 0.0625
- up_weight: bfloat16 [4, 7168, 1024], P('ep', 'sub'), may hold values from -0.0625 to 0.0625
- down_weight: bfloat16 [4, 1024, 7168], P('ep', None, 'sub'), may hold values from -0.1875 to 0.1875
- shared_gate: bfloat16 [1024, 7168], P('ep', 'sub'), may hold values from -0.0625 to 0.0625
- shared_up: bfloat16 [1024, 7168], P('ep', 'sub'), may hold values from -0.0625 to 0.0625
- shared_down: bfloat16 [1024, 7168], P('ep', 'sub'), may hold values from -0.1875 to 0.1875
Outputs:
- layer_out: bfloat16 [512, 7168], P(('groups', 'ep'), 'sub'), parts along dimension 0
The draws below stay inside these ranges and needn't reach their ends.
There are 2 independent parts, one for each index of `groups`. The reference program is written for one: setup_inputs(seed, part) draws one part's arguments, and reference() takes and returns one part's arrays. A program takes and returns all parts, laid end to end along the dimension named above; an argument that names none is the same for every part. Nothing has to cross between parts.
Inputs may be any that keep to these rules, and one draw needn't show every extreme that they name: `expert_ids`: each row names 2 different experts. Among the 64 rows of one ep index no expert is named more than 48 times, and in some of these aligned blocks an expert is named exactly 48 times.
All inputs are finite; a program needn't handle non-finite values.
Results may differ from the reference program's by a relative error of at most 0.0054.
Values may be sent and summed in bfloat16 or wider, within the bound.
A program may use at most 128 MiB of HBM per device.

```python
import math
import jax
import jax.numpy as jnp
import numpy as np
from jax import lax

D = 7168
HIDDEN_SIZE = 1024
SH = 1024
TOK_EP = 64
EXPERTS = 4
TOPK = 2
CAP = 48
TOKENS = 256
N_EP = 4


def level_of(stream_key, shape, pieces, least, largest):
    def one(dim, shards_of):
        steps = jax.random.uniform(jax.random.fold_in(jax.random.fold_in(stream_key, 6), dim), (shards_of,), jnp.float32, least / len(pieces), largest / len(pieces))
        return jnp.repeat(jnp.exp(steps), shape[dim] // shards_of).reshape((-1,) + (1,) * (len(shape) - dim - 1))

    gain = one(*pieces[0])
    for cut in pieces[1:]:
        gain = gain * one(*cut)
    return gain


def deal_out(stream_key, own, number, rows, count, top, limit, lean):
    order = jax.random.permutation(stream_key, count)
    heavy_load, ordinary = portions_of(count, rows * top, limit, lean, True), portions_of(count, rows * top, limit, lean, False)
    places = jnp.arange(count)

    def named(lengths, offset_by):
        used = int((lengths > 0).sum())
        fixed = max(1, used // 4)
        moved = fixed + (places - fixed + offset_by * (used - fixed)) % max(1, count - fixed)
        return jnp.zeros((count,), jnp.int32).at[order[jnp.where(places < fixed, places, moved)]].set(jnp.asarray(lengths, jnp.int32))

    lengths = jnp.where(number % 4 == 0, named(heavy_load, number // 4), named(ordinary, number - number // 4 - 1))
    mixed = jax.random.permutation(jax.random.fold_in(own, 3), count)
    giver, sink = mixed[0:count // 2 * 2:2], mixed[1:count // 2 * 2:2]
    slack = jnp.minimum(lengths[giver] - 1, limit - lengths[sink]) // 2
    slack = jnp.where((giver == order[0]) | (sink == order[0]) | (lengths[sink] == 0), 0, jnp.maximum(slack, 0))
    moved = jax.random.randint(jax.random.fold_in(own, 4), (count // 2,), 0, 1 << 20) % (slack + 1)
    lengths = lengths.at[giver].add(-moved).at[sink].add(moved)
    labels = jnp.searchsorted(jnp.cumsum(lengths), jnp.arange(rows * top), side="right").astype(jnp.int32)
    grid = labels.reshape(top, rows).T
    grid = grid[jax.random.permutation(jax.random.fold_in(own, 1), rows)]
    offset_by = jax.random.randint(jax.random.fold_in(own, 2), (rows, 1), 0, top)
    return jnp.take_along_axis(grid, (jnp.arange(top)[None, :] + offset_by) % top, axis=1)


def portions_of(number_of, total, bound, lean, full):
    loads = [(1 << 20) // math.isqrt(rank ** lean) + 1 for rank in range(1, number_of + 1)]
    largest = bound if full else min(bound, max(-(-total // number_of), total * loads[0] // sum(loads)))
    least = 1 if total - largest >= number_of - 1 else 0
    counts, spare = [largest] + [least] * (number_of - 1), total - largest - least * (number_of - 1)
    while spare > 0:
        movable = [i for i in range(1, number_of) if counts[i] < largest] or [i for i in range(1, number_of) if counts[i] < bound]
        mass, left = sum([loads[i] for i in movable]), spare
        for i in movable:
            extra = min(bound - counts[i], max(1, left * loads[i] // mass), spare)
            counts[i] = counts[i] + extra
            spare = spare - extra
    return np.array(counts)


def centred(stream_key, extent, width, reach, split=(), kind=jnp.bfloat16):
    gain = level_of(stream_key, extent, split, -0.22, 0.18) if split else 1.0
    values = jax.random.normal(stream_key, extent, jnp.float32) * width * gain
    return jnp.minimum(jnp.maximum(values, -reach), reach).astype(kind)


def setup_inputs(seed: int = 0, part: int = 0) -> dict:
    key_of = jax.random.split(jax.random.key(seed), 10)
    part_keys = jax.random.split(jax.random.fold_in(key_of[9], part), 10)
    tokens = centred(part_keys[0], (TOKENS, D), 1.0, 6.0, ((0, 4), (1, 4)))
    expert_ids_keys = jax.random.split(jax.random.fold_in(part_keys[1], 1), TOKENS // TOK_EP)
    expert_ids_turns = jax.random.permutation(jax.random.fold_in(part_keys[1], 3), TOKENS // TOK_EP)
    expert_ids = jax.vmap(lambda own, number: deal_out(jax.random.fold_in(part_keys[1], 2), own, number, TOK_EP, EXPERTS, TOPK, CAP, 2))(expert_ids_keys, expert_ids_turns).reshape((TOKENS, TOPK))
    route_weights = jnp.clip(jnp.exp(math.log(0.6) - 2.4849067 * jax.random.uniform(part_keys[2], (TOKENS, TOPK), jnp.float32) ** level_of(part_keys[2], (TOKENS, TOPK), ((0, 4),), -0.2, 0.2)), 0.05, 0.6)
    gate_weight = centred(key_of[3], (EXPERTS, D, HIDDEN_SIZE), D ** -0.5, 0.0625, ((0, 4), (1, 4)))
    up_weight = centred(key_of[4], (EXPERTS, D, HIDDEN_SIZE), D ** -0.5, 0.0625, ((0, 4), (1, 4)))
    down_weight = centred(key_of[5], (EXPERTS, HIDDEN_SIZE, D), HIDDEN_SIZE ** -0.5, 0.1875, ((0, 4), (2, 4)))
    shared_gate = centred(key_of[6], (SH, D), D ** -0.5, 0.0625, ((0, 4), (1, 4)))
    shared_up = centred(key_of[7], (SH, D), D ** -0.5, 0.0625, ((0, 4), (1, 4)))
    shared_down = centred(key_of[8], (SH, D), SH ** -0.5, 0.1875, ((0, 4), (1, 4)))
    return {"tokens": tokens, "expert_ids": expert_ids, "route_weights": route_weights, "gate_weight": gate_weight, "up_weight": up_weight, "down_weight": down_weight, "shared_gate": shared_gate, "shared_up": shared_up, "shared_down": shared_down}


def reference(tokens, expert_ids, route_weights, gate_weight, up_weight, down_weight, shared_gate, shared_up, shared_down):
    contract = (((1,), (1,)), ((), ()))
    shared_pre = lax.dot_general(tokens, shared_gate, contract, preferred_element_type=jnp.float32)
    shared_lin = lax.dot_general(tokens, shared_up, contract, preferred_element_type=jnp.float32)
    shared_hidden = (jax.nn.silu(shared_pre) * shared_lin).astype(jnp.bfloat16)
    shared_out = jnp.dot(shared_hidden, shared_down, preferred_element_type=jnp.float32)
    most_rows = N_EP * CAP

    def expert_step(totals, inputs):
        gate_mat, up_mat, down_mat, expert = inputs
        chosen = expert_ids == expert
        weight_col = jnp.sum(jnp.where(chosen, route_weights, jnp.float32(0.0)), axis=1)
        absent = 1 - jnp.any(chosen, axis=1).astype(jnp.int32)
        row_order = jnp.argsort(absent, stable=True)[:most_rows].astype(jnp.int32)
        picked = tokens[row_order]
        expert_pre = jnp.dot(picked, gate_mat, preferred_element_type=jnp.float32)
        expert_lin = jnp.dot(picked, up_mat, preferred_element_type=jnp.float32)
        expert_hidden = (jax.nn.silu(expert_pre) * expert_lin).astype(jnp.bfloat16)
        expert_out = jnp.dot(expert_hidden, down_mat, preferred_element_type=jnp.float32).astype(jnp.bfloat16)
        totals = totals.at[row_order].add(weight_col[row_order][:, None] * expert_out.astype(jnp.float32))
        return totals, None

    expert_index = jnp.arange(EXPERTS, dtype=jnp.int32)
    routed, unused = lax.scan(expert_step, jnp.zeros((TOKENS, D), jnp.float32), (gate_weight, up_weight, down_weight, expert_index))
    return (shared_out + routed).astype(jnp.bfloat16)
```

```python
import functools

import jax
import jax.numpy as jnp
from jax import lax
from jax.experimental import pallas as pl
from jax.experimental.pallas import tpu as pltpu
from jax.sharding import PartitionSpec as P

MESH = pl.DeviceIdType.MESH
F32 = jnp.float32
BF16 = jnp.bfloat16
NT = (((1,), (1,)), ((), ()))
TN = (((0,), (0,)), ((), ()))


def dot(a, b, dims=None):
    if dims is None:
        return jnp.dot(a, b, preferred_element_type=F32)
    return lax.dot_general(a, b, dims, preferred_element_type=F32)


def mirrored(me, step, count):
    total, bit = 0, 1
    while bit < count:
        total = total + ((me // bit + step // bit) % 2) * bit
        bit *= 2
    return total


def silu(v):
    return v / (1.0 + jnp.exp(-v))


def kernel(
    n, ns, top, tok, meta, gw, uw, dw, sg, su, sd, out,
    toks, metas, gv, uv, dv, sgv, suv, sdv,
    hp, hr, sp, sr, own, hidr, hids, place, wslot, cs, cr, acc,
    w_sem, tok_ss, tok_rs, meta_ss, meta_rs, hp_ss, hp_rs, sp_ss, sp_rs,
    hr_ss, hr_rs, hs_ss, hs_rs, cs_ss, cs_rs, fw_ss,
):
    me, mq = lax.axis_index("ep"), lax.axis_index("sub")
    rows, width = tok.shape
    slots = place.shape[1]
    piece = hp.shape[-1]
    part = sp.shape[-2]
    chunk = 256 if width % 256 == 0 else 128

    line = n == 4
    inner = ((me + 1) // 2) % 2 if line else me * 0

    def turn(i):
        return lax.rem(i + inner, n)

    weights = [
        pltpu.make_async_copy(src, dst, w_sem.at[i])
        for i, (src, dst) in enumerate(
            [(sg, sgv), (su, suv), (gw.at[0], gv), (uw.at[0], uv), (sd, sdv), (dw.at[0], dv)]
        )
    ]
    for copy in weights:
        copy.start()

    def peer(d):
        return lax.rem(mq + d, ns)

    def partner(s):
        return mirrored(me, s, n)

    def remote(src, dst, ss, rs, where):
        return pltpu.make_async_remote_copy(
            src_ref=src, dst_ref=dst, send_sem=ss, recv_sem=rs,
            device_id=where, device_id_type=MESH,
        )

    def tok_copy(s):
        return remote(tok, toks.at[s], tok_ss.at[s], tok_rs.at[s], {"ep": partner(s)})

    def forward_copy():
        return remote(
            toks.at[2], toks.at[3], fw_ss.at[0], tok_rs.at[3], {"ep": partner(1)}
        )

    def meta_copy(s):
        return remote(meta, metas.at[s], meta_ss.at[s], meta_rs.at[s], {"ep": partner(s)})

    def hp_copy(s, d):
        return remote(
            hp.at[s, d - 1], hr.at[s, d - 1], hp_ss.at[s, d - 1], hp_rs.at[s, d - 1],
            {"sub": peer(d)},
        )

    def sp_copy(s, d):
        return remote(
            sp.at[s, peer(d)], sr.at[s, d - 1], sp_ss.at[s, d - 1], sp_rs.at[s, d - 1],
            {"sub": peer(d)},
        )

    def hr_copy(s, d):
        return remote(
            hidr.at[s, mq], hidr.at[s, mq], hr_ss.at[s, d - 1], hr_rs.at[s, d - 1],
            {"sub": peer(d)},
        )

    def hs_copy(s, d):
        return remote(
            hids.at[s, mq], hids.at[s, mq], hs_ss.at[s, d - 1], hs_rs.at[s, d - 1],
            {"sub": peer(d)},
        )

    def cs_copy(s):
        return remote(cs.at[s], cr.at[s], cs_ss.at[s], cs_rs.at[s], {"ep": partner(s)})

    def loop(first, last, body):
        if last - first <= 8:
            for s in range(first, last):
                body(s)
        else:
            lax.fori_loop(first, last, lambda s, c: (body(s), c)[1], 0)

    barrier = pltpu.get_barrier_semaphore()
    loop(1, n, lambda s: pl.semaphore_signal(
        barrier, inc=1, device_id={"ep": partner(s)}, device_id_type=MESH))
    for d in range(1, ns):
        pl.semaphore_signal(barrier, inc=1, device_id={"sub": peer(d)}, device_id_type=MESH)
    pl.semaphore_wait(barrier, n - 1 + ns - 1)

    def send_tokens(s):
        meta_copy(s).start()
        if line and s == 3:
            pl.when(inner == 1)(lambda: tok_copy(s).start())
        else:
            tok_copy(s).start()

    loop(1, n, send_tokens)
    toks[0] = tok[...]
    metas[0] = meta[...]

    def project(i):
        s = turn(i)

        @pl.when(s > 0)
        def _():
            meta_copy(s).wait_recv()
            tok_copy(s).wait_recv()

        if line and isinstance(i, int) and i == 1:
            pl.when(inner == 1)(lambda: forward_copy().start())
        first = isinstance(i, int) and i == 0
        if first:
            for copy in weights[:2]:
                copy.wait()
        block, info = toks.at[s], metas[s]
        gate = dot(block[...], sgv[...], NT)
        sp[i, :, 0] = gate.astype(BF16).reshape(ns, part, -1)
        up = dot(block[...], suv[...], NT)
        sp[i, :, 1] = up.astype(BF16).reshape(ns, part, -1)
        for d in range(1, ns):
            sp_copy(i, d).start()

        hit = (info[:top, :rows] == me.astype(F32)).astype(F32)
        member = jnp.sum(hit, axis=0, keepdims=True)
        weight = jnp.sum(hit * info[top:2 * top, :rows], axis=0, keepdims=True)
        before = (
            lax.broadcasted_iota(jnp.int32, (rows, rows), 0)
            < lax.broadcasted_iota(jnp.int32, (rows, rows), 1)
        ).astype(F32).astype(BF16)
        rank = dot(jnp.broadcast_to(member, (16, rows)).astype(BF16), before)[:1]
        spot = lax.broadcasted_iota(jnp.int32, (slots, rows), 0).astype(F32)
        placing = (spot == rank).astype(F32) * member
        wslot[i] = jnp.sum(placing * weight, axis=1, keepdims=True)
        placing = placing.astype(BF16)
        place[i] = placing
        picked = dot(placing, block[...]).astype(BF16)
        if first:
            for copy in weights[2:4]:
                copy.wait()
        for d in list(range(1, ns)) + [0]:
            cols = pl.ds(pl.multiple_of(peer(d) * piece, piece), piece)
            gate = dot(picked, gv[:, cols])
            up = dot(picked, uv[:, cols])
            if d:
                hp[i, d - 1, 0] = gate.astype(BF16)
                hp[i, d - 1, 1] = up.astype(BF16)
                hp_copy(i, d).start()
            else:
                own[i, 0] = gate
                own[i, 1] = up

    def activate(i):
        pre, lin = sp[i, mq, 0].astype(F32), sp[i, mq, 1].astype(F32)
        for d in range(1, ns):
            sp_copy(i, d).wait_recv()
            pre = pre + sr[i, d - 1, 0].astype(F32)
            lin = lin + sr[i, d - 1, 1].astype(F32)
        hids[i, mq] = (silu(pre) * lin).astype(BF16)
        for d in range(1, ns):
            hs_copy(i, d).start()
        pre, lin = own[i, 0], own[i, 1]
        for d in range(1, ns):
            hp_copy(i, d).wait_recv()
            pre = pre + hr[i, d - 1, 0].astype(F32)
            lin = lin + hr[i, d - 1, 1].astype(F32)
        hidr[i, mq] = (silu(pre) * lin).astype(BF16)
        for d in range(1, ns):
            hr_copy(i, d).start()

    def finish(i):
        s = turn(i)
        if isinstance(i, int) and i == 0:
            for copy in weights[4:]:
                copy.wait()
        for d in range(1, ns):
            hs_copy(i, d).wait_recv()
            hr_copy(i, d).wait_recv()
        hidden = jnp.concatenate([hidr[i, q] for q in range(ns)], axis=1)
        shared = hids[i].reshape(rows, -1)
        placing = place[i]
        scale = wslot[i]

        def columns(c, carry):
            cols = pl.ds(pl.multiple_of(c * chunk, chunk), chunk)
            routed = (dot(hidden, dv[:, cols]) * scale).astype(BF16)
            total = dot(placing, routed, TN) + dot(shared, sdv[:, cols])

            @pl.when(s == 0)
            def _():
                acc[:, cols] = total

            @pl.when(s > 0)
            def _():
                cs[s, :, cols] = total.astype(BF16)

            return carry

        lax.fori_loop(0, width // chunk, columns, 0)
        pl.when(s > 0)(lambda: cs_copy(s).start())

    project(0)
    activate(0)
    project(1)
    finish(0)
    activate(1)

    def step(s):
        project(s)
        finish(s - 1)
        activate(s)

    loop(2, n, step)
    finish(n - 1)

    def collect(s):
        cs_copy(s).wait_recv()
        acc[...] += cr[s].astype(F32)

    loop(1, n, collect)
    out[...] = acc[...].astype(out.dtype)

    def drain(s):
        if line and s == 3:
            @pl.when(inner == 1)
            def _():
                tok_copy(s).wait_send()
                forward_copy().wait_send()
        else:
            tok_copy(s).wait_send()
        meta_copy(s).wait_send()
        cs_copy(s).wait_send()

    loop(1, n, drain)

    def drain_sub(s):
        for d in range(1, ns):
            hp_copy(s, d).wait_send()
            sp_copy(s, d).wait_send()
            hr_copy(s, d).wait_send()
            hs_copy(s, d).wait_send()

    loop(0, n, drain_sub)


def per_device(tokens, expert_ids, route_weights, gate_weight, up_weight, down_weight,
               shared_gate, shared_up, shared_down):
    n, ns = lax.axis_size("ep"), lax.axis_size("sub")
    rows, width = tokens.shape
    top = expert_ids.shape[1]
    hidden = gate_weight.shape[2]
    local = shared_gate.shape[0]
    capacity = rows * top * 3 // (2 * n)
    slots = -(-capacity // 16) * 16
    piece, part = hidden // ns, rows // ns
    meta = jnp.concatenate([expert_ids.astype(F32), route_weights], axis=1).T
    meta = jnp.pad(meta, ((0, -(2 * top) % 8), (0, -rows % 128)))
    dma = pltpu.SemaphoreType.DMA
    vmem = pl.BlockSpec(memory_space=pltpu.VMEM)
    hbm = pl.BlockSpec(memory_space=pl.ANY)
    return pl.pallas_call(
        functools.partial(kernel, n, ns, top),
        out_shape=jax.ShapeDtypeStruct((rows, width), BF16),
        in_specs=[vmem] * 2 + [hbm] * 6,
        out_specs=vmem,
        scratch_shapes=[
            pltpu.VMEM((n, rows, width), BF16),
            pltpu.VMEM((n,) + meta.shape, F32),
            pltpu.VMEM((width, hidden), BF16),
            pltpu.VMEM((width, hidden), BF16),
            pltpu.VMEM((hidden, width), BF16),
            pltpu.VMEM((local, width), BF16),
            pltpu.VMEM((local, width), BF16),
            pltpu.VMEM((local, width), BF16),
            pltpu.VMEM((n, ns - 1, 2, slots, piece), BF16),
            pltpu.VMEM((n, ns - 1, 2, slots, piece), BF16),
            pltpu.VMEM((n, ns, 2, part, local), BF16),
            pltpu.VMEM((n, ns - 1, 2, part, local), BF16),
            pltpu.VMEM((n, 2, slots, piece), F32),
            pltpu.VMEM((n, ns, slots, piece), BF16),
            pltpu.VMEM((n, ns, part, local), BF16),
            pltpu.VMEM((n, slots, rows), BF16),
            pltpu.VMEM((n, slots, 1), F32),
            pltpu.VMEM((n, rows, width), BF16),
            pltpu.VMEM((n, rows, width), BF16),
            pltpu.VMEM((rows, width), F32),
            dma((6,)),
            dma((n,)), dma((n,)), dma((n,)), dma((n,)),
            dma((n, ns - 1)), dma((n, ns - 1)), dma((n, ns - 1)), dma((n, ns - 1)),
            dma((n, ns - 1)), dma((n, ns - 1)), dma((n, ns - 1)), dma((n, ns - 1)),
            dma((n,)), dma((n,)), dma((1,)),
        ],
        compiler_params=pltpu.CompilerParams(collective_id=0, has_side_effects=True),
    )(tokens, meta, gate_weight, up_weight, down_weight, shared_gate, shared_up, shared_down)

def line_kernel(
    n, ns, top, tok, ids, rw, gw, uw, dw, sg, su, sd, acc, cr,
    toks, metas, idv, rwv, gv, uv, dv, sguv, sdv, wcol, part, peer, own, xs, xr, hid, cs,
    w_sem, in_sem, tok_ss, tok_rs, meta_ss, meta_rs, d_ss, d_rs, x_ss, x_rs, h_ss, h_rs,
    c_ss, c_rs,
):
    me, mq = lax.axis_index("ep"), lax.axis_index("sub")
    rows, width = tok.shape
    half_rows = rows // 2
    hh, ll = gv.shape[1] // 2, sguv.shape[1] // 2
    chunk = 256 if width % 256 == 0 else 128
    core = lax.rem(mq, 2)
    mate = mq + 1 - 2 * core
    across = lax.rem(mq + 2, ns)
    sign = 1 - 2 * (me // 2)
    inner = ((me + 1) // 2) % 2
    source = [me, me + sign * (1 - 2 * inner), me + sign * (2 - inner), me + sign * (3 - inner)]
    units = [(0, 0, rows), (1, 0, rows), (2, 0, rows), (3, 0, half_rows), (3, half_rows, half_rows)]
    pieces = [pl.ds(0, hh), pl.ds(hh, hh), pl.ds(2 * hh, 2 * ll)]

    def remote(src, dst, ss, rs, where):
        return pltpu.make_async_remote_copy(
            src_ref=src, dst_ref=dst, send_sem=ss, recv_sem=rs,
            device_id=where, device_id_type=MESH,
        )

    def on_inner(body):
        pl.when(inner == 1)(body)

    def on_edge(body):
        pl.when(inner == 0)(body)

    inputs = [
        pltpu.make_async_copy(tok, toks.at[me], in_sem.at[0]),
        pltpu.make_async_copy(ids, idv, in_sem.at[1]),
        pltpu.make_async_copy(rw, rwv, in_sem.at[2]),
    ]
    weights = [
        pltpu.make_async_copy(gw.at[0], gv, w_sem.at[0]),
        pltpu.make_async_copy(uw.at[0], uv, w_sem.at[1]),
    ]
    for h in range(2):
        for j, src in enumerate((sg, su)):
            weights.append(pltpu.make_async_copy(
                src.at[pl.ds(h * ll, ll)], sguv.at[h, pl.ds(j * ll, ll)], w_sem.at[2 + 2 * h + j]))
    weights.append(pltpu.make_async_copy(dw.at[0], dv, w_sem.at[6]))
    weights.append(pltpu.make_async_copy(sd, sdv, w_sem.at[7]))
    for copy in inputs + weights:
        copy.start()

    barrier = pltpu.get_barrier_semaphore()
    pl.semaphore_signal(barrier, inc=1, device_id={"ep": me + sign}, device_id_type=MESH)
    on_inner(lambda: pl.semaphore_signal(
        barrier, inc=1, device_id={"ep": me - sign}, device_id_type=MESH))
    pl.semaphore_signal(barrier, inc=1, device_id={"sub": mate}, device_id_type=MESH)
    pl.semaphore_signal(barrier, inc=1, device_id={"sub": across}, device_id_type=MESH)
    pl.semaphore_wait(barrier, 3 + inner)

    def tok_copy(s, h, away):
        block = toks.at[s, pl.ds(h * half_rows, half_rows)]
        return remote(block, block, tok_ss.at[s, h, away], tok_rs.at[s, h],
                      {"ep": me + sign * (1 - 2 * away)})

    def meta_copy(s, away):
        return remote(metas.at[s], metas.at[s], meta_ss.at[s, away], meta_rs.at[s],
                      {"ep": me + sign * (1 - 2 * away)})

    def mate_copy(u, j):
        m = units[u][2]
        return remote(part.at[u, pl.ds(0, m), pieces[j]], peer.at[u, pl.ds(0, m), pieces[j]],
                      d_ss.at[u, j], d_rs.at[u, j], {"sub": mate})

    def across_copy(u):
        m = units[u][2]
        return remote(xs.at[u, pl.ds(0, m)], xr.at[u, pl.ds(0, m)], x_ss.at[u], x_rs.at[u],
                      {"sub": across})

    def hid_copy(u):
        block = hid.at[u, core, pl.ds(0, units[u][2])]
        return remote(block, block, h_ss.at[u], h_rs.at[u], {"sub": mate})

    def out_copy(k, h):
        s, where = source[k], pl.ds(h * half_rows, half_rows)
        slot = lax.rem(me - s + n, n) - 1
        return remote(cs.at[k - 1, where], cr.at[slot, where], c_ss.at[k - 1, h],
                      c_rs.at[slot, h], {"ep": s})

    inputs[0].wait()
    for h in range(2):
        on_inner(lambda h=h: tok_copy(me, h, 1).start())
        tok_copy(me, h, 0).start()
    inputs[1].wait()
    inputs[2].wait()
    metas[me] = jnp.zeros(metas.shape[1:], F32)
    for e in range(n):
        metas[me, e:e + 1, :rows] = jnp.sum(
            jnp.where(idv[...] == e, rwv[...], 0.0), axis=0, keepdims=True)
    on_inner(lambda: meta_copy(me, 1).start())
    meta_copy(me, 0).start()

    def take(k, halves):
        if 0 in halves:
            meta_copy(source[k], 0).wait_recv()
        for h in halves:
            tok_copy(source[k], h, 0).wait_recv()

    def forward(k, h, away):
        s = source[k]
        tok_copy(s, h, 0).wait_recv()
        tok_copy(s, h, away).start()
        if h == 0:
            meta_copy(s, 0).wait_recv()
            meta_copy(s, away).start()

    def project(u):
        k, first, m = units[u]
        block = toks.at[source[k], pl.ds(first, m)]
        mine = pl.ds(0, m)
        for side, dst in ((1 - core, part), (core, own)):
            cols = pl.ds(pl.multiple_of(side * hh, hh), hh)
            dst[u, mine, pieces[0]] = dot(block[...], gv[:, cols])
            if dst is part:
                mate_copy(u, 0).start()
            dst[u, mine, pieces[1]] = dot(block[...], uv[:, cols])
            if dst is part:
                mate_copy(u, 1).start()
            dst[u, mine, pieces[2]] = dot(block[...], sguv[side], NT)
            if dst is part:
                mate_copy(u, 2).start()

    def reduce(u):
        mine = pl.ds(0, units[u][2])
        for j, cols in enumerate(pieces):
            mate_copy(u, j).wait_recv()
            total = own[u, mine, cols] + peer[u, mine, cols]
            own[u, mine, cols] = total
            xs[u, mine, cols] = total.astype(BF16)
        across_copy(u).start()

    def activate(u):
        mine = pl.ds(0, units[u][2])
        across_copy(u).wait_recv()
        gate, up, shared = [own[u, mine, cols] + xr[u, mine, cols].astype(F32) for cols in pieces]
        hid[u, core, mine, pl.ds(0, hh)] = (silu(gate) * up).astype(BF16)
        hid[u, core, mine, pl.ds(hh, ll)] = (silu(shared[:, :ll]) * shared[:, ll:]).astype(BF16)
        hid_copy(u).start()

    def weigh(k):
        line = metas[source[k], pl.ds(me, 1), pl.ds(0, rows)]
        eye = (
            lax.broadcasted_iota(jnp.int32, (rows, rows), 0)
            == lax.broadcasted_iota(jnp.int32, (rows, rows), 1)
        )
        wcol[k] = jnp.sum(jnp.where(eye, line, 0.0), axis=1, keepdims=True)

    def finish(u):
        k, first, m = units[u]
        mine = pl.ds(0, m)
        scale = wcol[k, pl.ds(first, m)]
        hid_copy(u).wait_recv()
        routed = jnp.concatenate([hid[u, c, mine, pl.ds(0, hh)] for c in range(2)], axis=1)
        shared = jnp.concatenate([hid[u, c, mine, pl.ds(hh, ll)] for c in range(2)], axis=1)
        for c in range(width // chunk):
            cols = pl.ds(c * chunk, chunk)
            total = dot(routed, dv[:, cols]) * scale + dot(shared, sdv[:, cols])
            if k == 0:
                acc[:, cols] = total
            else:
                cs[k - 1, pl.ds(first, m), cols] = total.astype(BF16)
        if k:
            for h in range(first // half_rows, (first + m) // half_rows):
                out_copy(k, h).start()

    for copy in weights[:6]:
        copy.wait()
    project(0)

    @on_inner
    def _():
        forward(2, 0, 1)
        forward(1, 0, 0)

    weigh(0)
    reduce(0)

    @on_inner
    def _():
        forward(2, 1, 1)
        forward(1, 1, 0)

    on_edge(lambda: take(1, (0, 1)))
    project(1)
    weigh(1)
    reduce(1)
    on_inner(lambda: forward(3, 0, 1))
    activate(0)
    on_edge(lambda: take(2, (0, 1)))
    project(2)
    weigh(2)
    on_inner(lambda: forward(3, 1, 1))
    reduce(2)
    for copy in weights[6:]:
        copy.wait()
    finish(0)
    activate(1)
    on_edge(lambda: take(3, (0,)))
    project(3)
    weigh(3)
    reduce(3)
    finish(1)
    on_edge(lambda: take(3, (1,)))
    project(4)
    reduce(4)
    activate(2)
    finish(2)
    activate(3)
    finish(3)
    activate(4)
    finish(4)

    for slot in range(n - 1):
        for h in range(2):
            where = pl.ds(h * half_rows, half_rows)
            remote(cs.at[slot, where], cr.at[slot, where], c_ss.at[slot, h], c_rs.at[slot, h],
                   {"ep": me + sign}).wait_recv()
    for k in range(1, n):
        for h in range(2):
            out_copy(k, h).wait_send()
    for u in range(len(units)):
        for j in range(len(pieces)):
            mate_copy(u, j).wait_send()
        across_copy(u).wait_send()
        hid_copy(u).wait_send()
    for h in range(2):
        tok_copy(me, h, 0).wait_send()
    meta_copy(me, 0).wait_send()

    @on_inner
    def _():
        meta_copy(me, 1).wait_send()
        for k, away in ((1, 0), (2, 1), (3, 1)):
            meta_copy(source[k], away).wait_send()
            for h in range(2):
                tok_copy(source[k], h, away).wait_send()
        for h in range(2):
            tok_copy(me, h, 1).wait_send()


def line_device(tokens, expert_ids, route_weights, gate_weight, up_weight, down_weight,
                shared_gate, shared_up, shared_down):
    n, ns = lax.axis_size("ep"), lax.axis_size("sub")
    rows, width = tokens.shape
    top = expert_ids.shape[1]
    hidden = gate_weight.shape[2]
    local = shared_gate.shape[0]
    both, units = hidden + local, 5
    dma = pltpu.SemaphoreType.DMA
    vmem = pl.BlockSpec(memory_space=pltpu.VMEM)
    hbm = pl.BlockSpec(memory_space=pl.ANY)
    total, sums = pl.pallas_call(
        functools.partial(line_kernel, n, ns, top),
        out_shape=(pltpu.VMEM((rows, width), F32), pltpu.VMEM((n - 1, rows, width), BF16)),
        in_specs=[hbm] * 9,
        out_specs=(vmem, vmem),
        scratch_shapes=[
            pltpu.VMEM((n, rows, width), BF16),
            pltpu.VMEM((n, -(-n // 8) * 8, -(-rows // 128) * 128), F32),
            pltpu.VMEM((top, rows), jnp.int32),
            pltpu.VMEM((top, rows), F32),
            pltpu.VMEM((width, hidden), BF16),
            pltpu.VMEM((width, hidden), BF16),
            pltpu.VMEM((hidden, width), BF16),
            pltpu.VMEM((2, local, width), BF16),
            pltpu.VMEM((local, width), BF16),
            pltpu.VMEM((n, rows, 1), F32),
            pltpu.VMEM((units, rows, both), F32),
            pltpu.VMEM((units, rows, both), F32),
            pltpu.VMEM((units, rows, both), F32),
            pltpu.VMEM((units, rows, both), BF16),
            pltpu.VMEM((units, rows, both), BF16),
            pltpu.VMEM((units, 2, rows, both // 2), BF16),
            pltpu.VMEM((n - 1, rows, width), BF16),
            dma((8,)), dma((3,)),
            dma((n, 2, 2)), dma((n, 2)), dma((n, 2)), dma((n,)),
            dma((units, 3)), dma((units, 3)), dma((units,)), dma((units,)),
            dma((units,)), dma((units,)), dma((n - 1, 2)), dma((n - 1, 2)),
        ],
        compiler_params=pltpu.CompilerParams(collective_id=0, has_side_effects=True),
    )(tokens, expert_ids.T, route_weights.T, gate_weight, up_weight, down_weight,
      shared_gate, shared_up, shared_down)
    for slot in range(n - 1):
        total = total + sums[slot].astype(F32)
    return total.astype(BF16)


def solution(mesh):
    in_specs = (
        P(("groups", "ep"), "sub"),
        P(("groups", "ep"), None),
        P(("groups", "ep"), None),
        P("ep", "sub", None),
        P("ep", "sub", None),
        P("ep", None, "sub"),
        P("ep", "sub"),
        P("ep", "sub"),
        P("ep", "sub"),
    )
    out_specs = P(("groups", "ep"), "sub")
    line = mesh.shape["ep"] == 4 and mesh.shape["sub"] == 4
    return jax.shard_map(
        line_device if line else per_device, mesh=mesh, in_specs=in_specs, out_specs=out_specs, check_vma=False
    )
```

```python
import functools

import jax
import jax.numpy as jnp
from jax import lax
from jax.experimental import pallas as pl
from jax.experimental.pallas import tpu as pltpu
from jax.sharding import PartitionSpec as P

MESH = pl.DeviceIdType.MESH
F32 = jnp.float32
BF16 = jnp.bfloat16
NT = (((1,), (1,)), ((), ()))
TN = (((0,), (0,)), ((), ()))


def dot(a, b, dims=None):
    if dims is None:
        return jnp.dot(a, b, preferred_element_type=F32)
    return lax.dot_general(a, b, dims, preferred_element_type=F32)


def mirrored(me, step, count):
    total, bit = 0, 1
    while bit < count:
        total = total + ((me // bit + step // bit) % 2) * bit
        bit *= 2
    return total


def silu(v):
    return v / (1.0 + jnp.exp(-v))


def kernel(
    n, ns, top, tok, meta, gw, uw, dw, sg, su, sd, out,
    toks, metas, gv, uv, dv, sgv, suv, sdv,
    hp, hr, sp, sr, own, hidr, hids, place, wslot, cs, cr, acc,
    w_sem, tok_ss, tok_rs, meta_ss, meta_rs, hp_ss, hp_rs, sp_ss, sp_rs,
    hr_ss, hr_rs, hs_ss, hs_rs, cs_ss, cs_rs, fw_ss,
):
    me, mq = lax.axis_index("ep"), lax.axis_index("sub")
    rows, width = tok.shape
    slots = place.shape[1]
    piece = hp.shape[-1]
    part = sp.shape[-2]
    chunk = 256 if width % 256 == 0 else 128

    line = n == 4
    inner = ((me + 1) // 2) % 2 if line else me * 0

    def turn(i):
        return lax.rem(i + inner, n)

    weights = [
        pltpu.make_async_copy(src, dst, w_sem.at[i])
        for i, (src, dst) in enumerate(
            [(sg, sgv), (su, suv), (gw.at[0], gv), (uw.at[0], uv), (sd, sdv), (dw.at[0], dv)]
        )
    ]
    for copy in weights:
        copy.start()

    def peer(d):
        return lax.rem(mq + d, ns)

    def partner(s):
        return mirrored(me, s, n)

    def remote(src, dst, ss, rs, where):
        return pltpu.make_async_remote_copy(
            src_ref=src, dst_ref=dst, send_sem=ss, recv_sem=rs,
            device_id=where, device_id_type=MESH,
        )

    def tok_copy(s):
        return remote(tok, toks.at[s], tok_ss.at[s], tok_rs.at[s], {"ep": partner(s)})

    def forward_copy():
        return remote(
            toks.at[2], toks.at[3], fw_ss.at[0], tok_rs.at[3], {"ep": partner(1)}
        )

    def meta_copy(s):
        return remote(meta, metas.at[s], meta_ss.at[s], meta_rs.at[s], {"ep": partner(s)})

    def hp_copy(s, d):
        return remote(
            hp.at[s, d - 1], hr.at[s, d - 1], hp_ss.at[s, d - 1], hp_rs.at[s, d - 1],
            {"sub": peer(d)},
        )

    def sp_copy(s, d):
        return remote(
            sp.at[s, peer(d)], sr.at[s, d - 1], sp_ss.at[s, d - 1], sp_rs.at[s, d - 1],
            {"sub": peer(d)},
        )

    def hr_copy(s, d):
        return remote(
            hidr.at[s, mq], hidr.at[s, mq], hr_ss.at[s, d - 1], hr_rs.at[s, d - 1],
            {"sub": peer(d)},
        )

    def hs_copy(s, d):
        return remote(
            hids.at[s, mq], hids.at[s, mq], hs_ss.at[s, d - 1], hs_rs.at[s, d - 1],
            {"sub": peer(d)},
        )

    def cs_copy(s):
        return remote(cs.at[s], cr.at[s], cs_ss.at[s], cs_rs.at[s], {"ep": partner(s)})

    def loop(first, last, body):
        if last - first <= 8:
            for s in range(first, last):
                body(s)
        else:
            lax.fori_loop(first, last, lambda s, c: (body(s), c)[1], 0)

    barrier = pltpu.get_barrier_semaphore()
    loop(1, n, lambda s: pl.semaphore_signal(
        barrier, inc=1, device_id={"ep": partner(s)}, device_id_type=MESH))
    for d in range(1, ns):
        pl.semaphore_signal(barrier, inc=1, device_id={"sub": peer(d)}, device_id_type=MESH)
    pl.semaphore_wait(barrier, n - 1 + ns - 1)

    def send_tokens(s):
        meta_copy(s).start()
        if line and s == 3:
            pl.when(inner == 1)(lambda: tok_copy(s).start())
        else:
            tok_copy(s).start()

    loop(1, n, send_tokens)
    toks[0] = tok[...]
    metas[0] = meta[...]

    def project(i):
        s = turn(i)

        @pl.when(s > 0)
        def _():
            meta_copy(s).wait_recv()
            tok_copy(s).wait_recv()

        if line and isinstance(i, int) and i == 1:
            pl.when(inner == 1)(lambda: forward_copy().start())
        first = isinstance(i, int) and i == 0
        if first:
            for copy in weights[:2]:
                copy.wait()
        block, info = toks.at[s], metas[s]
        gate = dot(block[...], sgv[...], NT)
        sp[i, :, 0] = gate.astype(BF16).reshape(ns, part, -1)
        up = dot(block[...], suv[...], NT)
        sp[i, :, 1] = up.astype(BF16).reshape(ns, part, -1)
        for d in range(1, ns):
            sp_copy(i, d).start()

        hit = (info[:top, :rows] == me.astype(F32)).astype(F32)
        member = jnp.sum(hit, axis=0, keepdims=True)
        weight = jnp.sum(hit * info[top:2 * top, :rows], axis=0, keepdims=True)
        before = (
            lax.broadcasted_iota(jnp.int32, (rows, rows), 0)
            < lax.broadcasted_iota(jnp.int32, (rows, rows), 1)
        ).astype(F32).astype(BF16)
        rank = dot(jnp.broadcast_to(member, (16, rows)).astype(BF16), before)[:1]
        spot = lax.broadcasted_iota(jnp.int32, (slots, rows), 0).astype(F32)
        placing = (spot == rank).astype(F32) * member
        wslot[i] = jnp.sum(placing * weight, axis=1, keepdims=True)
        placing = placing.astype(BF16)
        place[i] = placing
        picked = dot(placing, block[...]).astype(BF16)
        if first:
            for copy in weights[2:4]:
                copy.wait()
        for d in list(range(1, ns)) + [0]:
            cols = pl.ds(pl.multiple_of(peer(d) * piece, piece), piece)
            gate = dot(picked, gv[:, cols])
            up = dot(picked, uv[:, cols])
            if d:
                hp[i, d - 1, 0] = gate.astype(BF16)
                hp[i, d - 1, 1] = up.astype(BF16)
                hp_copy(i, d).start()
            else:
                own[i, 0] = gate
                own[i, 1] = up

    def activate(i):
        pre, lin = sp[i, mq, 0].astype(F32), sp[i, mq, 1].astype(F32)
        for d in range(1, ns):
            sp_copy(i, d).wait_recv()
            pre = pre + sr[i, d - 1, 0].astype(F32)
            lin = lin + sr[i, d - 1, 1].astype(F32)
        hids[i, mq] = (silu(pre) * lin).astype(BF16)
        for d in range(1, ns):
            hs_copy(i, d).start()
        pre, lin = own[i, 0], own[i, 1]
        for d in range(1, ns):
            hp_copy(i, d).wait_recv()
            pre = pre + hr[i, d - 1, 0].astype(F32)
            lin = lin + hr[i, d - 1, 1].astype(F32)
        hidr[i, mq] = (silu(pre) * lin).astype(BF16)
        for d in range(1, ns):
            hr_copy(i, d).start()

    def finish(i):
        s = turn(i)
        if isinstance(i, int) and i == 0:
            for copy in weights[4:]:
                copy.wait()
        for d in range(1, ns):
            hs_copy(i, d).wait_recv()
            hr_copy(i, d).wait_recv()
        hidden = jnp.concatenate([hidr[i, q] for q in range(ns)], axis=1)
        shared = hids[i].reshape(rows, -1)
        placing = place[i]
        scale = wslot[i]

        def columns(c, carry):
            cols = pl.ds(pl.multiple_of(c * chunk, chunk), chunk)
            routed = (dot(hidden, dv[:, cols]) * scale).astype(BF16)
            total = dot(placing, routed, TN) + dot(shared, sdv[:, cols])

            @pl.when(s == 0)
            def _():
                acc[:, cols] = total

            @pl.when(s > 0)
            def _():
                cs[s, :, cols] = total.astype(BF16)

            return carry

        lax.fori_loop(0, width // chunk, columns, 0)
        pl.when(s > 0)(lambda: cs_copy(s).start())

    project(0)
    activate(0)
    project(1)
    finish(0)
    activate(1)

    def step(s):
        project(s)
        finish(s - 1)
        activate(s)

    loop(2, n, step)
    finish(n - 1)

    def collect(s):
        cs_copy(s).wait_recv()
        acc[...] += cr[s].astype(F32)

    loop(1, n, collect)
    out[...] = acc[...].astype(out.dtype)

    def drain(s):
        if line and s == 3:
            @pl.when(inner == 1)
            def _():
                tok_copy(s).wait_send()
                forward_copy().wait_send()
        else:
            tok_copy(s).wait_send()
        meta_copy(s).wait_send()
        cs_copy(s).wait_send()

    loop(1, n, drain)

    def drain_sub(s):
        for d in range(1, ns):
            hp_copy(s, d).wait_send()
            sp_copy(s, d).wait_send()
            hr_copy(s, d).wait_send()
            hs_copy(s, d).wait_send()

    loop(0, n, drain_sub)


def per_device(tokens, expert_ids, route_weights, gate_weight, up_weight, down_weight,
               shared_gate, shared_up, shared_down):
    n, ns = lax.axis_size("ep"), lax.axis_size("sub")
    rows, width = tokens.shape
    top = expert_ids.shape[1]
    hidden = gate_weight.shape[2]
    local = shared_gate.shape[0]
    capacity = rows * top * 3 // (2 * n)
    slots = -(-capacity // 16) * 16
    piece, part = hidden // ns, rows // ns
    meta = jnp.concatenate([expert_ids.astype(F32), route_weights], axis=1).T
    meta = jnp.pad(meta, ((0, -(2 * top) % 8), (0, -rows % 128)))
    dma = pltpu.SemaphoreType.DMA
    vmem = pl.BlockSpec(memory_space=pltpu.VMEM)
    hbm = pl.BlockSpec(memory_space=pl.ANY)
    return pl.pallas_call(
        functools.partial(kernel, n, ns, top),
        out_shape=jax.ShapeDtypeStruct((rows, width), BF16),
        in_specs=[vmem] * 2 + [hbm] * 6,
        out_specs=vmem,
        scratch_shapes=[
            pltpu.VMEM((n, rows, width), BF16),
            pltpu.VMEM((n,) + meta.shape, F32),
            pltpu.VMEM((width, hidden), BF16),
            pltpu.VMEM((width, hidden), BF16),
            pltpu.VMEM((hidden, width), BF16),
            pltpu.VMEM((local, width), BF16),
            pltpu.VMEM((local, width), BF16),
            pltpu.VMEM((local, width), BF16),
            pltpu.VMEM((n, ns - 1, 2, slots, piece), BF16),
            pltpu.VMEM((n, ns - 1, 2, slots, piece), BF16),
            pltpu.VMEM((n, ns, 2, part, local), BF16),
            pltpu.VMEM((n, ns - 1, 2, part, local), BF16),
            pltpu.VMEM((n, 2, slots, piece), F32),
            pltpu.VMEM((n, ns, slots, piece), BF16),
            pltpu.VMEM((n, ns, part, local), BF16),
            pltpu.VMEM((n, slots, rows), BF16),
            pltpu.VMEM((n, slots, 1), F32),
            pltpu.VMEM((n, rows, width), BF16),
            pltpu.VMEM((n, rows, width), BF16),
            pltpu.VMEM((rows, width), F32),
            dma((6,)),
            dma((n,)), dma((n,)), dma((n,)), dma((n,)),
            dma((n, ns - 1)), dma((n, ns - 1)), dma((n, ns - 1)), dma((n, ns - 1)),
            dma((n, ns - 1)), dma((n, ns - 1)), dma((n, ns - 1)), dma((n, ns - 1)),
            dma((n,)), dma((n,)), dma((1,)),
        ],
        compiler_params=pltpu.CompilerParams(collective_id=0, has_side_effects=True),
    )(tokens, meta, gate_weight, up_weight, down_weight, shared_gate, shared_up, shared_down)

def line_kernel(
    n, ns, top, tok, ids, rw, gw, uw, dw, sg, su, sd, acc, cr,
    toks, metas, idv, rwv, gv, uv, dv, sgv, suv, sdv, turned, part, peer, own, xs, xr, hid, cs,
    w_sem, in_sem, tok_ss, tok_rs, meta_ss, meta_rs, d_ss, d_rs, x_ss, x_rs, h_ss, h_rs,
    c_ss, c_rs,
):
    me, mq = lax.axis_index("ep"), lax.axis_index("sub")
    rows, width = tok.shape
    half = rows // 2
    hh, ll = gv.shape[1] // 2, sgv.shape[0] // 2
    chunk = 256 if width % 256 == 0 else 128
    core = lax.rem(mq, 2)
    mate = mq + 1 - 2 * core
    across = lax.rem(mq + 2, ns)
    sign = 1 - 2 * (me // 2)
    inner = ((me + 1) // 2) % 2
    steps = [0, 1, 1 - 2 * inner, 2 - inner, 2 - 3 * inner, 3 - inner, 3 - inner]
    source = [me + sign * step for step in steps]
    parity = [0, 0, 1 - inner, inner, 1, 0, 1]
    size = [rows] + [half] * 6
    pieces = [pl.ds(0, hh), pl.ds(hh, hh), pl.ds(2 * hh, 2 * ll)]

    def span(h):
        return pl.ds(h * half if isinstance(h, int) else pl.multiple_of(h * half, half), half)

    def place(u):
        return pl.ds(0, rows) if u == 0 else span(parity[u])

    def remote(src, dst, ss, rs, where):
        return pltpu.make_async_remote_copy(
            src_ref=src, dst_ref=dst, send_sem=ss, recv_sem=rs,
            device_id=where, device_id_type=MESH,
        )

    def on_inner(body):
        pl.when(inner == 1)(body)

    def on_edge(body):
        pl.when(inner == 0)(body)

    inputs = [
        pltpu.make_async_copy(tok, toks.at[me], in_sem.at[0]),
        pltpu.make_async_copy(ids, idv, in_sem.at[1]),
        pltpu.make_async_copy(rw, rwv, in_sem.at[2]),
    ]
    weights = [
        pltpu.make_async_copy(src, dst, w_sem.at[i])
        for i, (src, dst) in enumerate(
            [(sg, sgv), (su, suv), (gw.at[0], gv), (uw.at[0], uv), (dw.at[0], dv), (sd, sdv)]
        )
    ]
    for copy in inputs + weights[:4]:
        copy.start()

    barrier = pltpu.get_barrier_semaphore()
    pl.semaphore_signal(barrier, inc=1, device_id={"ep": me + sign}, device_id_type=MESH)
    on_inner(lambda: pl.semaphore_signal(
        barrier, inc=1, device_id={"ep": me - sign}, device_id_type=MESH))
    pl.semaphore_signal(barrier, inc=1, device_id={"sub": mate}, device_id_type=MESH)
    pl.semaphore_signal(barrier, inc=1, device_id={"sub": across}, device_id_type=MESH)
    pl.semaphore_wait(barrier, 3 + inner)

    def tok_copy(s, h, away):
        block = toks.at[s, span(h)]
        return remote(block, block, tok_ss.at[s, h, away], tok_rs.at[s, h],
                      {"ep": me + sign * (1 - 2 * away)})

    def meta_copy(s, away):
        return remote(metas.at[s], metas.at[s], meta_ss.at[s, away], meta_rs.at[s],
                      {"ep": me + sign * (1 - 2 * away)})

    def mate_copy(u, j):
        mine = pl.ds(0, size[u])
        return remote(part.at[u, mine, pieces[j]], peer.at[u, mine, pieces[j]],
                      d_ss.at[u, j], d_rs.at[u, j], {"sub": mate})

    def across_copy(u):
        mine = pl.ds(0, size[u])
        return remote(xs.at[u, mine], xr.at[u, mine], x_ss.at[u], x_rs.at[u], {"sub": across})

    def hid_copy(u):
        block = hid.at[u, core, pl.ds(0, size[u])]
        return remote(block, block, h_ss.at[u], h_rs.at[u], {"sub": mate})

    def out_copy(u):
        slot = lax.rem(me - source[u] + n, n) - 1
        return remote(cs.at[u - 1], cr.at[slot, place(u)], c_ss.at[u - 1],
                      c_rs.at[slot, parity[u]], {"ep": source[u]})

    inputs[0].wait()
    for h in range(2):
        on_inner(lambda h=h: tok_copy(me, h, 1).start())
        tok_copy(me, h, 0).start()
    inputs[1].wait()
    inputs[2].wait()
    metas[me] = jnp.zeros(metas.shape[1:], F32)
    for e in range(n):
        metas[me, e:e + 1, :rows] = jnp.sum(
            jnp.where(idv[...] == e, rwv[...], 0.0), axis=0, keepdims=True)
    on_inner(lambda: meta_copy(me, 1).start())
    meta_copy(me, 0).start()

    def take(u):
        def wait():
            tok_copy(source[u], parity[u], 0).wait_recv()
            if u % 2:
                meta_copy(source[u], 0).wait_recv()

        on_edge(wait)

    def forward(u, away):
        def send():
            s, h = source[u], parity[u]
            tok_copy(s, h, 0).wait_recv()
            tok_copy(s, h, away).start()
            if u in (1, 2, 5):
                meta_copy(s, 0).wait_recv()
                meta_copy(s, away).start()

        on_inner(send)

    def project(u):
        mine = pl.ds(0, size[u])
        block = toks.at[source[u], place(u)]
        for side, dst in ((1 - core, part), (core, own)):
            cols = pl.ds(pl.multiple_of(side * hh, hh), hh)
            values = (
                lambda: dot(block[...], gv[:, cols]),
                lambda: dot(block[...], uv[:, cols]),
                lambda: dot(block[...], turned[side]),
            )
            for j, value in enumerate(values):
                dst[u, mine, pieces[j]] = value()
                if dst is part:
                    mate_copy(u, j).start()

    def reduce(u):
        mine = pl.ds(0, size[u])
        for j, cols in enumerate(pieces):
            mate_copy(u, j).wait_recv()
            total = own[u, mine, cols] + peer[u, mine, cols]
            own[u, mine, cols] = total
            xs[u, mine, cols] = total.astype(BF16)
        across_copy(u).start()

    def activate(u):
        mine = pl.ds(0, size[u])
        across_copy(u).wait_recv()
        gate, up, shared = [own[u, mine, cols] + xr[u, mine, cols].astype(F32) for cols in pieces]
        hid[u, core, mine, pl.ds(0, hh)] = (silu(gate) * up).astype(BF16)
        hid[u, core, mine, pl.ds(hh, ll)] = (silu(shared[:, :ll]) * shared[:, ll:]).astype(BF16)
        hid_copy(u).start()

    def finish(u):
        m = size[u]
        mine = pl.ds(0, m)
        line = metas[source[u], pl.ds(me, 1), pl.ds(0, rows)]
        row = lax.broadcasted_iota(jnp.int32, (m, rows), 0) + parity[u] * half
        eye = row == lax.broadcasted_iota(jnp.int32, (m, rows), 1)
        scale = jnp.sum(jnp.where(eye, line, 0.0), axis=1, keepdims=True)
        hid_copy(u).wait_recv()
        routed = jnp.concatenate([hid[u, c, mine, pl.ds(0, hh)] for c in range(2)], axis=1)
        shared = jnp.concatenate([hid[u, c, mine, pl.ds(hh, ll)] for c in range(2)], axis=1)
        for c in range(width // chunk):
            cols = pl.ds(c * chunk, chunk)
            total = dot(routed, dv[:, cols]) * scale + dot(shared, sdv[:, cols])
            if u == 0:
                acc[:, cols] = total
            else:
                cs[u - 1, :, cols] = total.astype(BF16)
        if u:
            out_copy(u).start()

    for copy in weights[:2]:
        copy.wait()
    for side in range(2):
        for j, src in enumerate((sgv, suv)):
            turned[side, :, j * ll:(j + 1) * ll] = src[side * ll:(side + 1) * ll, :].T
    for copy in weights[2:4]:
        copy.wait()
    for copy in weights[4:]:
        copy.start()
    project(0)
    forward(1, 1)
    forward(2, 0)
    reduce(0)
    take(1)
    project(1)
    reduce(1)
    forward(3, 1)
    forward(4, 0)
    take(2)
    project(2)
    reduce(2)
    forward(5, 1)
    take(3)
    project(3)
    activate(0)
    activate(1)
    reduce(3)
    forward(6, 1)
    take(4)
    project(4)
    for copy in weights[4:]:
        copy.wait()
    finish(1)
    activate(2)
    reduce(4)
    take(5)
    project(5)
    finish(2)
    activate(3)
    reduce(5)
    take(6)
    project(6)
    finish(3)
    activate(4)
    reduce(6)
    finish(4)
    activate(5)
    finish(5)
    activate(6)
    finish(6)
    finish(0)

    for slot in range(n - 1):
        for h in range(2):
            remote(cs.at[0], cr.at[slot, span(h)], c_ss.at[0], c_rs.at[slot, h],
                   {"ep": me + sign}).wait_recv()
    for u in range(len(size)):
        if u:
            out_copy(u).wait_send()
        for j in range(len(pieces)):
            mate_copy(u, j).wait_send()
        across_copy(u).wait_send()
        hid_copy(u).wait_send()
    for h in range(2):
        tok_copy(me, h, 0).wait_send()
    meta_copy(me, 0).wait_send()

    @on_inner
    def _():
        meta_copy(me, 1).wait_send()
        for h in range(2):
            tok_copy(me, h, 1).wait_send()
        for u, away in ((1, 1), (2, 0), (3, 1), (4, 0), (5, 1), (6, 1)):
            tok_copy(source[u], parity[u], away).wait_send()
            if u in (1, 2, 5):
                meta_copy(source[u], away).wait_send()


def line_device(tokens, expert_ids, route_weights, gate_weight, up_weight, down_weight,
                shared_gate, shared_up, shared_down):
    n, ns = lax.axis_size("ep"), lax.axis_size("sub")
    rows, width = tokens.shape
    top = expert_ids.shape[1]
    hidden = gate_weight.shape[2]
    local = shared_gate.shape[0]
    both, units = hidden + local, 7
    dma = pltpu.SemaphoreType.DMA
    vmem = pl.BlockSpec(memory_space=pltpu.VMEM)
    hbm = pl.BlockSpec(memory_space=pl.ANY)
    total, sums = pl.pallas_call(
        functools.partial(line_kernel, n, ns, top),
        out_shape=(pltpu.VMEM((rows, width), F32), pltpu.VMEM((n - 1, rows, width), BF16)),
        in_specs=[hbm] * 9,
        out_specs=(vmem, vmem),
        scratch_shapes=[
            pltpu.VMEM((n, rows, width), BF16),
            pltpu.VMEM((n, -(-n // 8) * 8, -(-rows // 128) * 128), F32),
            pltpu.VMEM((top, rows), jnp.int32),
            pltpu.VMEM((top, rows), F32),
            pltpu.VMEM((width, hidden), BF16),
            pltpu.VMEM((width, hidden), BF16),
            pltpu.VMEM((hidden, width), BF16),
            pltpu.VMEM((local, width), BF16),
            pltpu.VMEM((local, width), BF16),
            pltpu.VMEM((local, width), BF16),
            pltpu.VMEM((2, width, local), BF16),
            pltpu.VMEM((units, rows, both), F32),
            pltpu.VMEM((units, rows, both), F32),
            pltpu.VMEM((units, rows, both), F32),
            pltpu.VMEM((units, rows, both), BF16),
            pltpu.VMEM((units, rows, both), BF16),
            pltpu.VMEM((units, 2, rows, both // 2), BF16),
            pltpu.VMEM((units - 1, rows // 2, width), BF16),
            dma((6,)), dma((3,)),
            dma((n, 2, 2)), dma((n, 2)), dma((n, 2)), dma((n,)),
            dma((units, 3)), dma((units, 3)), dma((units,)), dma((units,)),
            dma((units,)), dma((units,)), dma((units - 1,)), dma((n - 1, 2)),
        ],
        compiler_params=pltpu.CompilerParams(collective_id=0, has_side_effects=True),
    )(tokens, expert_ids.T, route_weights.T, gate_weight, up_weight, down_weight,
      shared_gate, shared_up, shared_down)
    for slot in range(n - 1):
        total = total + sums[slot].astype(F32)
    return total.astype(BF16)


def solution(mesh):
    in_specs = (
        P(("groups", "ep"), "sub"),
        P(("groups", "ep"), None),
        P(("groups", "ep"), None),
        P("ep", "sub", None),
        P("ep", "sub", None),
        P("ep", None, "sub"),
        P("ep", "sub"),
        P("ep", "sub"),
        P("ep", "sub"),
    )
    out_specs = P(("groups", "ep"), "sub")
    line = mesh.shape["ep"] == 4 and mesh.shape["sub"] == 4
    return jax.shard_map(
        line_device if line else per_device, mesh=mesh, in_specs=in_specs, out_specs=out_specs, check_vma=False
    )
```

```python
import functools

import jax
import jax.numpy as jnp
from jax import lax
from jax.experimental import pallas as pl
from jax.experimental.pallas import tpu as pltpu
from jax.sharding import PartitionSpec as P

MESH = pl.DeviceIdType.MESH
F32 = jnp.float32
BF16 = jnp.bfloat16
NT = (((1,), (1,)), ((), ()))
TN = (((0,), (0,)), ((), ()))


def dot(a, b, dims=None):
    if dims is None:
        return jnp.dot(a, b, preferred_element_type=F32)
    return lax.dot_general(a, b, dims, preferred_element_type=F32)


def mirrored(me, step, count):
    total, bit = 0, 1
    while bit < count:
        total = total + ((me // bit + step // bit) % 2) * bit
        bit *= 2
    return total


def silu(v):
    return v / (1.0 + jnp.exp(-v))


def kernel(
    n, ns, top, tok, meta, gw, uw, dw, sg, su, sd, out,
    toks, metas, gv, uv, dv, sgv, suv, sdv,
    hp, hr, sp, sr, own, hidr, hids, place, wslot, cs, cr, acc,
    w_sem, tok_ss, tok_rs, meta_ss, meta_rs, hp_ss, hp_rs, sp_ss, sp_rs,
    hr_ss, hr_rs, hs_ss, hs_rs, cs_ss, cs_rs, fw_ss,
):
    me, mq = lax.axis_index("ep"), lax.axis_index("sub")
    rows, width = tok.shape
    slots = place.shape[1]
    piece = hp.shape[-1]
    part = sp.shape[-2]
    chunk = 256 if width % 256 == 0 else 128

    line = n == 4
    inner = ((me + 1) // 2) % 2 if line else me * 0

    def turn(i):
        return lax.rem(i + inner, n)

    weights = [
        pltpu.make_async_copy(src, dst, w_sem.at[i])
        for i, (src, dst) in enumerate(
            [(sg, sgv), (su, suv), (gw.at[0], gv), (uw.at[0], uv), (sd, sdv), (dw.at[0], dv)]
        )
    ]
    for copy in weights:
        copy.start()

    def peer(d):
        return lax.rem(mq + d, ns)

    def partner(s):
        return mirrored(me, s, n)

    def remote(src, dst, ss, rs, where):
        return pltpu.make_async_remote_copy(
            src_ref=src, dst_ref=dst, send_sem=ss, recv_sem=rs,
            device_id=where, device_id_type=MESH,
        )

    def tok_copy(s):
        return remote(tok, toks.at[s], tok_ss.at[s], tok_rs.at[s], {"ep": partner(s)})

    def forward_copy():
        return remote(
            toks.at[2], toks.at[3], fw_ss.at[0], tok_rs.at[3], {"ep": partner(1)}
        )

    def meta_copy(s):
        return remote(meta, metas.at[s], meta_ss.at[s], meta_rs.at[s], {"ep": partner(s)})

    def hp_copy(s, d):
        return remote(
            hp.at[s, d - 1], hr.at[s, d - 1], hp_ss.at[s, d - 1], hp_rs.at[s, d - 1],
            {"sub": peer(d)},
        )

    def sp_copy(s, d):
        return remote(
            sp.at[s, peer(d)], sr.at[s, d - 1], sp_ss.at[s, d - 1], sp_rs.at[s, d - 1],
            {"sub": peer(d)},
        )

    def hr_copy(s, d):
        return remote(
            hidr.at[s, mq], hidr.at[s, mq], hr_ss.at[s, d - 1], hr_rs.at[s, d - 1],
            {"sub": peer(d)},
        )

    def hs_copy(s, d):
        return remote(
            hids.at[s, mq], hids.at[s, mq], hs_ss.at[s, d - 1], hs_rs.at[s, d - 1],
            {"sub": peer(d)},
        )

    def cs_copy(s):
        return remote(cs.at[s], cr.at[s], cs_ss.at[s], cs_rs.at[s], {"ep": partner(s)})

    def loop(first, last, body):
        if last - first <= 8:
            for s in range(first, last):
                body(s)
        else:
            lax.fori_loop(first, last, lambda s, c: (body(s), c)[1], 0)

    barrier = pltpu.get_barrier_semaphore()
    loop(1, n, lambda s: pl.semaphore_signal(
        barrier, inc=1, device_id={"ep": partner(s)}, device_id_type=MESH))
    for d in range(1, ns):
        pl.semaphore_signal(barrier, inc=1, device_id={"sub": peer(d)}, device_id_type=MESH)
    pl.semaphore_wait(barrier, n - 1 + ns - 1)

    def send_tokens(s):
        meta_copy(s).start()
        if line and s == 3:
            pl.when(inner == 1)(lambda: tok_copy(s).start())
        else:
            tok_copy(s).start()

    loop(1, n, send_tokens)
    toks[0] = tok[...]
    metas[0] = meta[...]

    def project(i):
        s = turn(i)

        @pl.when(s > 0)
        def _():
            meta_copy(s).wait_recv()
            tok_copy(s).wait_recv()

        if line and isinstance(i, int) and i == 1:
            pl.when(inner == 1)(lambda: forward_copy().start())
        first = isinstance(i, int) and i == 0
        if first:
            for copy in weights[:2]:
                copy.wait()
        block, info = toks.at[s], metas[s]
        gate = dot(block[...], sgv[...], NT)
        sp[i, :, 0] = gate.astype(BF16).reshape(ns, part, -1)
        up = dot(block[...], suv[...], NT)
        sp[i, :, 1] = up.astype(BF16).reshape(ns, part, -1)
        for d in range(1, ns):
            sp_copy(i, d).start()

        hit = (info[:top, :rows] == me.astype(F32)).astype(F32)
        member = jnp.sum(hit, axis=0, keepdims=True)
        weight = jnp.sum(hit * info[top:2 * top, :rows], axis=0, keepdims=True)
        before = (
            lax.broadcasted_iota(jnp.int32, (rows, rows), 0)
            < lax.broadcasted_iota(jnp.int32, (rows, rows), 1)
        ).astype(F32).astype(BF16)
        rank = dot(jnp.broadcast_to(member, (16, rows)).astype(BF16), before)[:1]
        spot = lax.broadcasted_iota(jnp.int32, (slots, rows), 0).astype(F32)
        placing = (spot == rank).astype(F32) * member
        wslot[i] = jnp.sum(placing * weight, axis=1, keepdims=True)
        placing = placing.astype(BF16)
        place[i] = placing
        picked = dot(placing, block[...]).astype(BF16)
        if first:
            for copy in weights[2:4]:
                copy.wait()
        for d in list(range(1, ns)) + [0]:
            cols = pl.ds(pl.multiple_of(peer(d) * piece, piece), piece)
            gate = dot(picked, gv[:, cols])
            up = dot(picked, uv[:, cols])
            if d:
                hp[i, d - 1, 0] = gate.astype(BF16)
                hp[i, d - 1, 1] = up.astype(BF16)
                hp_copy(i, d).start()
            else:
                own[i, 0] = gate
                own[i, 1] = up

    def activate(i):
        pre, lin = sp[i, mq, 0].astype(F32), sp[i, mq, 1].astype(F32)
        for d in range(1, ns):
            sp_copy(i, d).wait_recv()
            pre = pre + sr[i, d - 1, 0].astype(F32)
            lin = lin + sr[i, d - 1, 1].astype(F32)
        hids[i, mq] = (silu(pre) * lin).astype(BF16)
        for d in range(1, ns):
            hs_copy(i, d).start()
        pre, lin = own[i, 0], own[i, 1]
        for d in range(1, ns):
            hp_copy(i, d).wait_recv()
            pre = pre + hr[i, d - 1, 0].astype(F32)
            lin = lin + hr[i, d - 1, 1].astype(F32)
        hidr[i, mq] = (silu(pre) * lin).astype(BF16)
        for d in range(1, ns):
            hr_copy(i, d).start()

    def finish(i):
        s = turn(i)
        if isinstance(i, int) and i == 0:
            for copy in weights[4:]:
                copy.wait()
        for d in range(1, ns):
            hs_copy(i, d).wait_recv()
            hr_copy(i, d).wait_recv()
        hidden = jnp.concatenate([hidr[i, q] for q in range(ns)], axis=1)
        shared = hids[i].reshape(rows, -1)
        placing = place[i]
        scale = wslot[i]

        def columns(c, carry):
            cols = pl.ds(pl.multiple_of(c * chunk, chunk), chunk)
            routed = (dot(hidden, dv[:, cols]) * scale).astype(BF16)
            total = dot(placing, routed, TN) + dot(shared, sdv[:, cols])

            @pl.when(s == 0)
            def _():
                acc[:, cols] = total

            @pl.when(s > 0)
            def _():
                cs[s, :, cols] = total.astype(BF16)

            return carry

        lax.fori_loop(0, width // chunk, columns, 0)
        pl.when(s > 0)(lambda: cs_copy(s).start())

    project(0)
    activate(0)
    project(1)
    finish(0)
    activate(1)

    def step(s):
        project(s)
        finish(s - 1)
        activate(s)

    loop(2, n, step)
    finish(n - 1)

    def collect(s):
        cs_copy(s).wait_recv()
        acc[...] += cr[s].astype(F32)

    loop(1, n, collect)
    out[...] = acc[...].astype(out.dtype)

    def drain(s):
        if line and s == 3:
            @pl.when(inner == 1)
            def _():
                tok_copy(s).wait_send()
                forward_copy().wait_send()
        else:
            tok_copy(s).wait_send()
        meta_copy(s).wait_send()
        cs_copy(s).wait_send()

    loop(1, n, drain)

    def drain_sub(s):
        for d in range(1, ns):
            hp_copy(s, d).wait_send()
            sp_copy(s, d).wait_send()
            hr_copy(s, d).wait_send()
            hs_copy(s, d).wait_send()

    loop(0, n, drain_sub)


def per_device(tokens, expert_ids, route_weights, gate_weight, up_weight, down_weight,
               shared_gate, shared_up, shared_down):
    n, ns = lax.axis_size("ep"), lax.axis_size("sub")
    rows, width = tokens.shape
    top = expert_ids.shape[1]
    hidden = gate_weight.shape[2]
    local = shared_gate.shape[0]
    capacity = rows * top * 3 // (2 * n)
    slots = -(-capacity // 16) * 16
    piece, part = hidden // ns, rows // ns
    meta = jnp.concatenate([expert_ids.astype(F32), route_weights], axis=1).T
    meta = jnp.pad(meta, ((0, -(2 * top) % 8), (0, -rows % 128)))
    dma = pltpu.SemaphoreType.DMA
    vmem = pl.BlockSpec(memory_space=pltpu.VMEM)
    hbm = pl.BlockSpec(memory_space=pl.ANY)
    return pl.pallas_call(
        functools.partial(kernel, n, ns, top),
        out_shape=jax.ShapeDtypeStruct((rows, width), BF16),
        in_specs=[vmem] * 2 + [hbm] * 6,
        out_specs=vmem,
        scratch_shapes=[
            pltpu.VMEM((n, rows, width), BF16),
            pltpu.VMEM((n,) + meta.shape, F32),
            pltpu.VMEM((width, hidden), BF16),
            pltpu.VMEM((width, hidden), BF16),
            pltpu.VMEM((hidden, width), BF16),
            pltpu.VMEM((local, width), BF16),
            pltpu.VMEM((local, width), BF16),
            pltpu.VMEM((local, width), BF16),
            pltpu.VMEM((n, ns - 1, 2, slots, piece), BF16),
            pltpu.VMEM((n, ns - 1, 2, slots, piece), BF16),
            pltpu.VMEM((n, ns, 2, part, local), BF16),
            pltpu.VMEM((n, ns - 1, 2, part, local), BF16),
            pltpu.VMEM((n, 2, slots, piece), F32),
            pltpu.VMEM((n, ns, slots, piece), BF16),
            pltpu.VMEM((n, ns, part, local), BF16),
            pltpu.VMEM((n, slots, rows), BF16),
            pltpu.VMEM((n, slots, 1), F32),
            pltpu.VMEM((n, rows, width), BF16),
            pltpu.VMEM((n, rows, width), BF16),
            pltpu.VMEM((rows, width), F32),
            dma((6,)),
            dma((n,)), dma((n,)), dma((n,)), dma((n,)),
            dma((n, ns - 1)), dma((n, ns - 1)), dma((n, ns - 1)), dma((n, ns - 1)),
            dma((n, ns - 1)), dma((n, ns - 1)), dma((n, ns - 1)), dma((n, ns - 1)),
            dma((n,)), dma((n,)), dma((1,)),
        ],
        compiler_params=pltpu.CompilerParams(collective_id=0, has_side_effects=True),
    )(tokens, meta, gate_weight, up_weight, down_weight, shared_gate, shared_up, shared_down)

def line_kernel(
    n, ns, top, tok, ids, rw, gw, uw, dw, sg, su, sd, acc, cr,
    toks, metas, idv, rwv, gv, uv, dv, sgv, suv, sdv, turned, part, peer, own, xs, xr, hid, cs, hold, joint,
    w_sem, in_sem, tok_ss, tok_rs, meta_ss, meta_rs, d_ss, d_rs, x_ss, x_rs, h_ss, h_rs,
    c_ss, c_rs, j_rs,
):
    me, mq = lax.axis_index("ep"), lax.axis_index("sub")
    rows, width = tok.shape
    half = rows // 2
    hh, ll = gv.shape[1] // 2, sgv.shape[0] // 2
    chunk = 256 if width % 256 == 0 else 128
    core = lax.rem(mq, 2)
    mate = mq + 1 - 2 * core
    across = lax.rem(mq + 2, ns)
    sign = 1 - 2 * (me // 2)
    inner = ((me + 1) // 2) % 2
    steps = [0, 1, 1, 2, 2, 3 - 4 * inner, 3 - 4 * inner]
    source = [me + sign * step for step in steps]
    parity = [0, 0, 1, 0, 1, 0, 1]
    size = [rows] + [half] * 6
    left = width // 2 // 128 * 128
    sides = [pl.ds(0, left), pl.ds(left, width - left)]
    pieces = [pl.ds(0, hh), pl.ds(hh, hh), pl.ds(2 * hh, 2 * ll)]

    def span(h):
        return pl.ds(h * half, half)

    def place(u):
        return pl.ds(0, rows) if u == 0 else span(parity[u])

    def remote(src, dst, ss, rs, where):
        return pltpu.make_async_remote_copy(
            src_ref=src, dst_ref=dst, send_sem=ss, recv_sem=rs,
            device_id=where, device_id_type=MESH,
        )

    def on_inner(body):
        pl.when(inner == 1)(body)

    def on_edge(body):
        pl.when(inner == 0)(body)

    inputs = [
        pltpu.make_async_copy(tok, toks.at[me], in_sem.at[0]),
        pltpu.make_async_copy(ids, idv, in_sem.at[1]),
        pltpu.make_async_copy(rw, rwv, in_sem.at[2]),
    ]
    weights = [
        pltpu.make_async_copy(src, dst, w_sem.at[i])
        for i, (src, dst) in enumerate(
            [(sg, sgv), (su, suv), (gw.at[0], gv), (uw.at[0], uv), (dw.at[0], dv), (sd, sdv)]
        )
    ]
    for copy in inputs:
        copy.start()

    barrier = pltpu.get_barrier_semaphore()
    pl.semaphore_signal(barrier, inc=1, device_id={"ep": me + sign}, device_id_type=MESH)
    on_inner(lambda: pl.semaphore_signal(
        barrier, inc=1, device_id={"ep": me - sign}, device_id_type=MESH))
    pl.semaphore_signal(barrier, inc=1, device_id={"sub": mate}, device_id_type=MESH)
    pl.semaphore_signal(barrier, inc=1, device_id={"sub": across}, device_id_type=MESH)

    def tok_copy(s, h, away):
        block = toks.at[s, span(h)]
        return remote(block, block, tok_ss.at[s, h, away], tok_rs.at[s, h],
                      {"ep": me + sign * (1 - 2 * away)})

    def meta_copy(s, away):
        return remote(metas.at[s], metas.at[s], meta_ss.at[s, away], meta_rs.at[s],
                      {"ep": me + sign * (1 - 2 * away)})

    def mate_copy(u):
        mine = pl.ds(0, size[u])
        return remote(part.at[u, mine], peer.at[u, mine], d_ss.at[u], d_rs.at[u], {"sub": mate})

    def across_copy(u):
        mine = pl.ds(0, size[u])
        return remote(xs.at[u, mine], xr.at[u, mine], x_ss.at[u], x_rs.at[u], {"sub": across})

    def hid_copy(u):
        block = hid.at[u, core, pl.ds(0, size[u])]
        return remote(block, block, h_ss.at[u], h_rs.at[u], {"sub": mate})

    def out_copy(u, c):
        slot = lax.rem(me - source[u] + n, n) - 1
        return remote(cs.at[u - 1, :, sides[c]], cr.at[slot, place(u), sides[c]],
                      c_ss.at[u - 1, c], c_rs.at[slot, parity[u], c], {"ep": source[u]})

    def far_copy(u, c):
        return remote(cs.at[u - 1, :, sides[c]], joint.at[u - 5, :, sides[c]],
                      c_ss.at[u - 1, c], j_rs.at[u - 5, c], {"ep": me + sign})

    inputs[1].wait()
    inputs[2].wait()
    metas[me] = jnp.zeros(metas.shape[1:], F32)
    for e in range(n):
        metas[me, e:e + 1, :rows] = jnp.sum(
            jnp.where(idv[...] == e, rwv[...], 0.0), axis=0, keepdims=True)
    inputs[0].wait()
    pl.semaphore_wait(barrier, 3 + inner)
    for h in range(2):
        on_inner(lambda h=h: tok_copy(me, h, 1).start())
        tok_copy(me, h, 0).start()
    on_inner(lambda: meta_copy(me, 1).start())
    meta_copy(me, 0).start()
    for copy in weights:
        copy.start()

    @on_edge
    def _():
        cr[lax.rem(source[5] - me + n, n) - 1] = jnp.zeros((rows, width), BF16)

    def take(u):
        def wait():
            tok_copy(source[u], parity[u], 0).wait_recv()
            if u % 2:
                meta_copy(source[u], 0).wait_recv()

        on_edge(wait)

    def forward(u, away):
        def send():
            s, h = source[u], parity[u]
            tok_copy(s, h, 0).wait_recv()
            tok_copy(s, h, away).start()
            if u % 2:
                meta_copy(s, 0).wait_recv()
                meta_copy(s, away).start()

        on_inner(send)

    def project(*group):
        block = jnp.concatenate([toks[source[v], place(v)] for v in group], axis=0)
        for side, dst in ((1 - core, part), (core, own)):
            cols = pl.ds(pl.multiple_of(side * hh, hh), hh)
            for j, matrix in enumerate((gv.at[:, cols], uv.at[:, cols], turned.at[side])):
                result, first = dot(block, matrix[...]), 0
                for v in group:
                    dst[v, pl.ds(0, size[v]), pieces[j]] = result[first:first + size[v]]
                    first += size[v]
            if dst is part:
                for v in group:
                    mate_copy(v).start()

    def reduce(u):
        mine = pl.ds(0, size[u])
        mate_copy(u).wait_recv()
        total = own[u, mine] + peer[u, mine]
        own[u, mine] = total
        xs[u, mine] = total.astype(BF16)
        across_copy(u).start()

    def activate(u):
        mine = pl.ds(0, size[u])
        across_copy(u).wait_recv()
        gate, up, shared = [own[u, mine, cols] + xr[u, mine, cols].astype(F32) for cols in pieces]
        hid[u, core, mine, pl.ds(0, hh)] = (silu(gate) * up).astype(BF16)
        hid[u, core, mine, pl.ds(hh, ll)] = (silu(shared[:, :ll]) * shared[:, ll:]).astype(BF16)
        hid_copy(u).start()

    def finish(*group):
        scales = []
        for v in group:
            m = size[v]
            line = metas[source[v], pl.ds(me, 1), pl.ds(0, rows)]
            row = lax.broadcasted_iota(jnp.int32, (m, rows), 0) + parity[v] * half
            eye = row == lax.broadcasted_iota(jnp.int32, (m, rows), 1)
            scales.append(jnp.sum(jnp.where(eye, line, 0.0), axis=1, keepdims=True))
        scale = jnp.concatenate(scales, axis=0)
        for v in group:
            hid_copy(v).wait_recv()
        routed, shared = [
            jnp.concatenate([
                jnp.concatenate([hid[v, c, pl.ds(0, size[v]), cols] for c in range(2)], axis=1)
                for v in group], axis=0)
            for cols in (pl.ds(0, hh), pl.ds(hh, ll))
        ]
        for c in range(width // chunk):
            cols = pl.ds(c * chunk, chunk)
            total, first = dot(routed, dv[:, cols]) * scale + dot(shared, sdv[:, cols]), 0
            for v in group:
                value = total[first:first + size[v]]
                first += size[v]
                if v == 0:
                    acc[:, cols] = value
                    continue
                cs[v - 1, :, cols] = value.astype(BF16)
                if v in (3, 4):
                    hold[v - 3, :, cols] = value

        def ship(v, copy):
            for c in range(2):
                copy(v, c).start()

        for v in group:
            if v in (1, 2):
                ship(v, out_copy)
            elif v in (3, 4):
                on_edge(lambda: ship(v, out_copy))
            elif v:
                on_edge(lambda: ship(v, far_copy))
                on_inner(lambda: ship(v, out_copy))

    def join(u, c):
        def add():
            far_copy(u + 2, c).wait_recv()
            cs[u - 1, :, sides[c]] = (
                hold[u - 3, :, sides[c]] + joint[u - 3, :, sides[c]].astype(F32)
            ).astype(BF16)
            out_copy(u, c).start()

        on_inner(add)

    for copy in weights[:2]:
        copy.wait()
    for side in range(2):
        for j, src in enumerate((sgv, suv)):
            turned[side, :, j * ll:(j + 1) * ll] = src[side * ll:(side + 1) * ll, :].T
    for copy in weights[2:4]:
        copy.wait()
    forward(1, 1)
    forward(5, 0)
    take(1)
    project(1, 0)
    reduce(1)
    forward(2, 1)
    forward(6, 0)
    take(2)
    project(2)
    reduce(2)
    forward(3, 1)
    take(3)
    project(3)
    activate(1)
    reduce(3)
    forward(4, 1)
    take(4)
    project(4)
    for copy in weights[4:]:
        copy.wait()
    finish(1)
    activate(2)
    reduce(4)
    take(5)
    project(5)
    finish(2)
    activate(3)
    reduce(5)
    take(6)
    project(6)
    finish(3)
    activate(4)
    reduce(6)
    reduce(0)
    finish(4)
    activate(5)
    finish(5)
    activate(6)
    activate(0)
    finish(6)
    finish(0)

    for u in (3, 4):
        for c in range(2):
            join(u, c)

    def landed(k):
        slot = lax.rem(source[k] - me + n, n) - 1
        for h in range(2):
            for c in range(2):
                remote(cs.at[0, :, sides[c]], cr.at[slot, span(h), sides[c]], c_ss.at[0, c],
                       c_rs.at[slot, h, c], {"ep": me + sign}).wait_recv()

    landed(1)
    landed(3)
    on_inner(lambda: landed(5))
    for u in range(len(size)):
        if u:
            for c in range(2):
                out_copy(u, c).wait_send()
        mate_copy(u).wait_send()
        across_copy(u).wait_send()
        hid_copy(u).wait_send()
    for h in range(2):
        tok_copy(me, h, 0).wait_send()
    meta_copy(me, 0).wait_send()

    @on_inner
    def _():
        meta_copy(me, 1).wait_send()
        for h in range(2):
            tok_copy(me, h, 1).wait_send()
        for u, away in ((1, 1), (2, 1), (3, 1), (4, 1), (5, 0), (6, 0)):
            tok_copy(source[u], parity[u], away).wait_send()
            if u % 2:
                meta_copy(source[u], away).wait_send()


def line_device(tokens, expert_ids, route_weights, gate_weight, up_weight, down_weight,
                shared_gate, shared_up, shared_down):
    n, ns = lax.axis_size("ep"), lax.axis_size("sub")
    rows, width = tokens.shape
    top = expert_ids.shape[1]
    hidden = gate_weight.shape[2]
    local = shared_gate.shape[0]
    both, units = hidden + local, 7
    dma = pltpu.SemaphoreType.DMA
    vmem = pl.BlockSpec(memory_space=pltpu.VMEM)
    hbm = pl.BlockSpec(memory_space=pl.ANY)
    total, sums = pl.pallas_call(
        functools.partial(line_kernel, n, ns, top),
        out_shape=(pltpu.VMEM((rows, width), F32), pltpu.VMEM((n - 1, rows, width), BF16)),
        in_specs=[hbm] * 9,
        out_specs=(vmem, vmem),
        scratch_shapes=[
            pltpu.VMEM((n, rows, width), BF16),
            pltpu.VMEM((n, -(-n // 8) * 8, -(-rows // 128) * 128), F32),
            pltpu.VMEM((top, rows), jnp.int32),
            pltpu.VMEM((top, rows), F32),
            pltpu.VMEM((width, hidden), BF16),
            pltpu.VMEM((width, hidden), BF16),
            pltpu.VMEM((hidden, width), BF16),
            pltpu.VMEM((local, width), BF16),
            pltpu.VMEM((local, width), BF16),
            pltpu.VMEM((local, width), BF16),
            pltpu.VMEM((2, width, local), BF16),
            pltpu.VMEM((units, rows, both), F32),
            pltpu.VMEM((units, rows, both), F32),
            pltpu.VMEM((units, rows, both), F32),
            pltpu.VMEM((units, rows, both), BF16),
            pltpu.VMEM((units, rows, both), BF16),
            pltpu.VMEM((units, 2, rows, both // 2), BF16),
            pltpu.VMEM((units - 1, rows // 2, width), BF16),
            pltpu.VMEM((2, rows // 2, width), F32),
            pltpu.VMEM((2, rows // 2, width), BF16),
            dma((6,)), dma((3,)),
            dma((n, 2, 2)), dma((n, 2)), dma((n, 2)), dma((n,)),
            dma((units,)), dma((units,)), dma((units,)), dma((units,)),
            dma((units,)), dma((units,)), dma((units - 1, 2)), dma((n - 1, 2, 2)), dma((2, 2)),
        ],
        compiler_params=pltpu.CompilerParams(collective_id=0, has_side_effects=True),
    )(tokens, expert_ids.T, route_weights.T, gate_weight, up_weight, down_weight,
      shared_gate, shared_up, shared_down)
    for slot in range(n - 1):
        total = total + sums[slot].astype(F32)
    return total.astype(BF16)


def solution(mesh):
    in_specs = (
        P(("groups", "ep"), "sub"),
        P(("groups", "ep"), None),
        P(("groups", "ep"), None),
        P("ep", "sub", None),
        P("ep", "sub", None),
        P("ep", None, "sub"),
        P("ep", "sub"),
        P("ep", "sub"),
        P("ep", "sub"),
    )
    out_specs = P(("groups", "ep"), "sub")
    line = mesh.shape["ep"] == 4 and mesh.shape["sub"] == 4
    return jax.shard_map(
        line_device if line else per_device, mesh=mesh, in_specs=in_specs, out_specs=out_specs, check_vma=False
    )
```

```python
import functools

import jax
import jax.numpy as jnp
from jax import lax
from jax.experimental import pallas as pl
from jax.experimental.pallas import tpu as pltpu
from jax.sharding import PartitionSpec as P

MESH = pl.DeviceIdType.MESH
F32 = jnp.float32
BF16 = jnp.bfloat16
NT = (((1,), (1,)), ((), ()))
TN = (((0,), (0,)), ((), ()))


def dot(a, b, dims=None):
    if dims is None:
        return jnp.dot(a, b, preferred_element_type=F32)
    return lax.dot_general(a, b, dims, preferred_element_type=F32)


def mirrored(me, step, count):
    total, bit = 0, 1
    while bit < count:
        total = total + ((me // bit + step // bit) % 2) * bit
        bit *= 2
    return total


def silu(v):
    return v / (1.0 + jnp.exp(-v))


def kernel(
    n, ns, top, tok, meta, gw, uw, dw, sg, su, sd, out,
    toks, metas, gv, uv, dv, sgv, suv, sdv,
    hp, hr, sp, sr, own, hidr, hids, place, wslot, cs, cr, acc,
    w_sem, tok_ss, tok_rs, meta_ss, meta_rs, hp_ss, hp_rs, sp_ss, sp_rs,
    hr_ss, hr_rs, hs_ss, hs_rs, cs_ss, cs_rs, fw_ss,
):
    me, mq = lax.axis_index("ep"), lax.axis_index("sub")
    rows, width = tok.shape
    slots = place.shape[1]
    piece = hp.shape[-1]
    part = sp.shape[-2]
    chunk = 256 if width % 256 == 0 else 128

    line = n == 4
    inner = ((me + 1) // 2) % 2 if line else me * 0

    def turn(i):
        return lax.rem(i + inner, n)

    weights = [
        pltpu.make_async_copy(src, dst, w_sem.at[i])
        for i, (src, dst) in enumerate(
            [(sg, sgv), (su, suv), (gw.at[0], gv), (uw.at[0], uv), (sd, sdv), (dw.at[0], dv)]
        )
    ]
    for copy in weights:
        copy.start()

    def peer(d):
        return lax.rem(mq + d, ns)

    def partner(s):
        return mirrored(me, s, n)

    def remote(src, dst, ss, rs, where):
        return pltpu.make_async_remote_copy(
            src_ref=src, dst_ref=dst, send_sem=ss, recv_sem=rs,
            device_id=where, device_id_type=MESH,
        )

    def tok_copy(s):
        return remote(tok, toks.at[s], tok_ss.at[s], tok_rs.at[s], {"ep": partner(s)})

    def forward_copy():
        return remote(
            toks.at[2], toks.at[3], fw_ss.at[0], tok_rs.at[3], {"ep": partner(1)}
        )

    def meta_copy(s):
        return remote(meta, metas.at[s], meta_ss.at[s], meta_rs.at[s], {"ep": partner(s)})

    def hp_copy(s, d):
        return remote(
            hp.at[s, d - 1], hr.at[s, d - 1], hp_ss.at[s, d - 1], hp_rs.at[s, d - 1],
            {"sub": peer(d)},
        )

    def sp_copy(s, d):
        return remote(
            sp.at[s, peer(d)], sr.at[s, d - 1], sp_ss.at[s, d - 1], sp_rs.at[s, d - 1],
            {"sub": peer(d)},
        )

    def hr_copy(s, d):
        return remote(
            hidr.at[s, mq], hidr.at[s, mq], hr_ss.at[s, d - 1], hr_rs.at[s, d - 1],
            {"sub": peer(d)},
        )

    def hs_copy(s, d):
        return remote(
            hids.at[s, mq], hids.at[s, mq], hs_ss.at[s, d - 1], hs_rs.at[s, d - 1],
            {"sub": peer(d)},
        )

    def cs_copy(s):
        return remote(cs.at[s], cr.at[s], cs_ss.at[s], cs_rs.at[s], {"ep": partner(s)})

    def loop(first, last, body):
        if last - first <= 8:
            for s in range(first, last):
                body(s)
        else:
            lax.fori_loop(first, last, lambda s, c: (body(s), c)[1], 0)

    barrier = pltpu.get_barrier_semaphore()
    loop(1, n, lambda s: pl.semaphore_signal(
        barrier, inc=1, device_id={"ep": partner(s)}, device_id_type=MESH))
    for d in range(1, ns):
        pl.semaphore_signal(barrier, inc=1, device_id={"sub": peer(d)}, device_id_type=MESH)
    pl.semaphore_wait(barrier, n - 1 + ns - 1)

    def send_tokens(s):
        meta_copy(s).start()
        if line and s == 3:
            pl.when(inner == 1)(lambda: tok_copy(s).start())
        else:
            tok_copy(s).start()

    loop(1, n, send_tokens)
    toks[0] = tok[...]
    metas[0] = meta[...]

    def project(i):
        s = turn(i)

        @pl.when(s > 0)
        def _():
            meta_copy(s).wait_recv()
            tok_copy(s).wait_recv()

        if line and isinstance(i, int) and i == 1:
            pl.when(inner == 1)(lambda: forward_copy().start())
        first = isinstance(i, int) and i == 0
        if first:
            for copy in weights[:2]:
                copy.wait()
        block, info = toks.at[s], metas[s]
        gate = dot(block[...], sgv[...], NT)
        sp[i, :, 0] = gate.astype(BF16).reshape(ns, part, -1)
        up = dot(block[...], suv[...], NT)
        sp[i, :, 1] = up.astype(BF16).reshape(ns, part, -1)
        for d in range(1, ns):
            sp_copy(i, d).start()

        hit = (info[:top, :rows] == me.astype(F32)).astype(F32)
        member = jnp.sum(hit, axis=0, keepdims=True)
        weight = jnp.sum(hit * info[top:2 * top, :rows], axis=0, keepdims=True)
        before = (
            lax.broadcasted_iota(jnp.int32, (rows, rows), 0)
            < lax.broadcasted_iota(jnp.int32, (rows, rows), 1)
        ).astype(F32).astype(BF16)
        rank = dot(jnp.broadcast_to(member, (16, rows)).astype(BF16), before)[:1]
        spot = lax.broadcasted_iota(jnp.int32, (slots, rows), 0).astype(F32)
        placing = (spot == rank).astype(F32) * member
        wslot[i] = jnp.sum(placing * weight, axis=1, keepdims=True)
        placing = placing.astype(BF16)
        place[i] = placing
        picked = dot(placing, block[...]).astype(BF16)
        if first:
            for copy in weights[2:4]:
                copy.wait()
        for d in list(range(1, ns)) + [0]:
            cols = pl.ds(pl.multiple_of(peer(d) * piece, piece), piece)
            gate = dot(picked, gv[:, cols])
            up = dot(picked, uv[:, cols])
            if d:
                hp[i, d - 1, 0] = gate.astype(BF16)
                hp[i, d - 1, 1] = up.astype(BF16)
                hp_copy(i, d).start()
            else:
                own[i, 0] = gate
                own[i, 1] = up

    def activate(i):
        pre, lin = sp[i, mq, 0].astype(F32), sp[i, mq, 1].astype(F32)
        for d in range(1, ns):
            sp_copy(i, d).wait_recv()
            pre = pre + sr[i, d - 1, 0].astype(F32)
            lin = lin + sr[i, d - 1, 1].astype(F32)
        hids[i, mq] = (silu(pre) * lin).astype(BF16)
        for d in range(1, ns):
            hs_copy(i, d).start()
        pre, lin = own[i, 0], own[i, 1]
        for d in range(1, ns):
            hp_copy(i, d).wait_recv()
            pre = pre + hr[i, d - 1, 0].astype(F32)
            lin = lin + hr[i, d - 1, 1].astype(F32)
        hidr[i, mq] = (silu(pre) * lin).astype(BF16)
        for d in range(1, ns):
            hr_copy(i, d).start()

    def finish(i):
        s = turn(i)
        if isinstance(i, int) and i == 0:
            for copy in weights[4:]:
                copy.wait()
        for d in range(1, ns):
            hs_copy(i, d).wait_recv()
            hr_copy(i, d).wait_recv()
        hidden = jnp.concatenate([hidr[i, q] for q in range(ns)], axis=1)
        shared = hids[i].reshape(rows, -1)
        placing = place[i]
        scale = wslot[i]

        def columns(c, carry):
            cols = pl.ds(pl.multiple_of(c * chunk, chunk), chunk)
            routed = (dot(hidden, dv[:, cols]) * scale).astype(BF16)
            total = dot(placing, routed, TN) + dot(shared, sdv[:, cols])

            @pl.when(s == 0)
            def _():
                acc[:, cols] = total

            @pl.when(s > 0)
            def _():
                cs[s, :, cols] = total.astype(BF16)

            return carry

        lax.fori_loop(0, width // chunk, columns, 0)
        pl.when(s > 0)(lambda: cs_copy(s).start())

    project(0)
    activate(0)
    project(1)
    finish(0)
    activate(1)

    def step(s):
        project(s)
        finish(s - 1)
        activate(s)

    loop(2, n, step)
    finish(n - 1)

    def collect(s):
        cs_copy(s).wait_recv()
        acc[...] += cr[s].astype(F32)

    loop(1, n, collect)
    out[...] = acc[...].astype(out.dtype)

    def drain(s):
        if line and s == 3:
            @pl.when(inner == 1)
            def _():
                tok_copy(s).wait_send()
                forward_copy().wait_send()
        else:
            tok_copy(s).wait_send()
        meta_copy(s).wait_send()
        cs_copy(s).wait_send()

    loop(1, n, drain)

    def drain_sub(s):
        for d in range(1, ns):
            hp_copy(s, d).wait_send()
            sp_copy(s, d).wait_send()
            hr_copy(s, d).wait_send()
            hs_copy(s, d).wait_send()

    loop(0, n, drain_sub)


def per_device(tokens, expert_ids, route_weights, gate_weight, up_weight, down_weight,
               shared_gate, shared_up, shared_down):
    n, ns = lax.axis_size("ep"), lax.axis_size("sub")
    rows, width = tokens.shape
    top = expert_ids.shape[1]
    hidden = gate_weight.shape[2]
    local = shared_gate.shape[0]
    capacity = rows * top * 3 // (2 * n)
    slots = -(-capacity // 16) * 16
    piece, part = hidden // ns, rows // ns
    meta = jnp.concatenate([expert_ids.astype(F32), route_weights], axis=1).T
    meta = jnp.pad(meta, ((0, -(2 * top) % 8), (0, -rows % 128)))
    dma = pltpu.SemaphoreType.DMA
    vmem = pl.BlockSpec(memory_space=pltpu.VMEM)
    hbm = pl.BlockSpec(memory_space=pl.ANY)
    return pl.pallas_call(
        functools.partial(kernel, n, ns, top),
        out_shape=jax.ShapeDtypeStruct((rows, width), BF16),
        in_specs=[vmem] * 2 + [hbm] * 6,
        out_specs=vmem,
        scratch_shapes=[
            pltpu.VMEM((n, rows, width), BF16),
            pltpu.VMEM((n,) + meta.shape, F32),
            pltpu.VMEM((width, hidden), BF16),
            pltpu.VMEM((width, hidden), BF16),
            pltpu.VMEM((hidden, width), BF16),
            pltpu.VMEM((local, width), BF16),
            pltpu.VMEM((local, width), BF16),
            pltpu.VMEM((local, width), BF16),
            pltpu.VMEM((n, ns - 1, 2, slots, piece), BF16),
            pltpu.VMEM((n, ns - 1, 2, slots, piece), BF16),
            pltpu.VMEM((n, ns, 2, part, local), BF16),
            pltpu.VMEM((n, ns - 1, 2, part, local), BF16),
            pltpu.VMEM((n, 2, slots, piece), F32),
            pltpu.VMEM((n, ns, slots, piece), BF16),
            pltpu.VMEM((n, ns, part, local), BF16),
            pltpu.VMEM((n, slots, rows), BF16),
            pltpu.VMEM((n, slots, 1), F32),
            pltpu.VMEM((n, rows, width), BF16),
            pltpu.VMEM((n, rows, width), BF16),
            pltpu.VMEM((rows, width), F32),
            dma((6,)),
            dma((n,)), dma((n,)), dma((n,)), dma((n,)),
            dma((n, ns - 1)), dma((n, ns - 1)), dma((n, ns - 1)), dma((n, ns - 1)),
            dma((n, ns - 1)), dma((n, ns - 1)), dma((n, ns - 1)), dma((n, ns - 1)),
            dma((n,)), dma((n,)), dma((1,)),
        ],
        compiler_params=pltpu.CompilerParams(collective_id=0, has_side_effects=True),
    )(tokens, meta, gate_weight, up_weight, down_weight, shared_gate, shared_up, shared_down)

def line_kernel(
    n, ns, top, tok, ids, rw, gw, uw, dw, sg, su, sd, acc, cr,
    toks, metas, idv, rwv, gv, uv, dv, sgv, suv, sdv, turned, part, peer, own, xs, xr, hid, cs, hold, joint,
    w_sem, in_sem, tok_ss, tok_rs, meta_ss, meta_rs, d_ss, d_rs, x_ss, x_rs, h_ss, h_rs,
    c_ss, c_rs, j_rs,
):
    me, mq = lax.axis_index("ep"), lax.axis_index("sub")
    rows, width = tok.shape
    half = rows // 2
    hh, ll = gv.shape[1] // 2, sgv.shape[0] // 2
    chunk = 256 if width % 256 == 0 else 128
    core = lax.rem(mq, 2)
    mate = mq + 1 - 2 * core
    across = lax.rem(mq + 2, ns)
    sign = 1 - 2 * (me // 2)
    inner = ((me + 1) // 2) % 2
    steps = [0, 1, 1, 2, 2, 3 - 4 * inner, 3 - 4 * inner]
    source = [me + sign * step for step in steps]
    parity = [0, 0, 1, 0, 1, 0, 1]
    size = [rows] + [half] * 6
    left = width // 2 // chunk * chunk
    sides = [pl.ds(0, left), pl.ds(left, width - left)]
    pieces = [pl.ds(0, hh), pl.ds(hh, hh), pl.ds(2 * hh, 2 * ll)]

    def span(h):
        return pl.ds(h * half, half)

    def place(u):
        return pl.ds(0, rows) if u == 0 else span(parity[u])

    def remote(src, dst, ss, rs, where):
        return pltpu.make_async_remote_copy(
            src_ref=src, dst_ref=dst, send_sem=ss, recv_sem=rs,
            device_id=where, device_id_type=MESH,
        )

    def on_inner(body):
        pl.when(inner == 1)(body)

    def on_edge(body):
        pl.when(inner == 0)(body)

    inputs = [
        pltpu.make_async_copy(tok, toks.at[me], in_sem.at[0]),
        pltpu.make_async_copy(ids, idv, in_sem.at[1]),
        pltpu.make_async_copy(rw, rwv, in_sem.at[2]),
    ]
    weights = [
        pltpu.make_async_copy(src, dst, w_sem.at[i])
        for i, (src, dst) in enumerate(
            [(sg, sgv), (su, suv), (gw.at[0], gv), (uw.at[0], uv), (dw.at[0], dv), (sd, sdv)]
        )
    ]
    for copy in inputs:
        copy.start()

    barrier = pltpu.get_barrier_semaphore()
    pl.semaphore_signal(barrier, inc=1, device_id={"ep": me + sign}, device_id_type=MESH)
    on_inner(lambda: pl.semaphore_signal(
        barrier, inc=1, device_id={"ep": me - sign}, device_id_type=MESH))
    pl.semaphore_signal(barrier, inc=1, device_id={"sub": mate}, device_id_type=MESH)
    pl.semaphore_signal(barrier, inc=1, device_id={"sub": across}, device_id_type=MESH)

    def tok_copy(s, h, away):
        block = toks.at[s, span(h)]
        return remote(block, block, tok_ss.at[s, h, away], tok_rs.at[s, h],
                      {"ep": me + sign * (1 - 2 * away)})

    def meta_copy(s, away):
        return remote(metas.at[s], metas.at[s], meta_ss.at[s, away], meta_rs.at[s],
                      {"ep": me + sign * (1 - 2 * away)})

    def mate_copy(u):
        mine = pl.ds(0, size[u])
        return remote(part.at[u, mine], peer.at[u, mine], d_ss.at[u], d_rs.at[u], {"sub": mate})

    def across_copy(u):
        mine = pl.ds(0, size[u])
        return remote(xs.at[u, mine], xr.at[u, mine], x_ss.at[u], x_rs.at[u], {"sub": across})

    def hid_copy(u):
        block = hid.at[u, core, pl.ds(0, size[u])]
        return remote(block, block, h_ss.at[u], h_rs.at[u], {"sub": mate})

    def out_copy(u, c):
        slot = lax.rem(me - source[u] + n, n) - 1
        return remote(cs.at[u - 1, :, sides[c]], cr.at[slot, place(u), sides[c]],
                      c_ss.at[u - 1, c], c_rs.at[slot, parity[u], c], {"ep": source[u]})

    def far_copy(u, c):
        return remote(cs.at[u - 1, :, sides[c]], joint.at[u - 5, :, sides[c]],
                      c_ss.at[u - 1, c], j_rs.at[u - 5, c], {"ep": me + sign})

    inputs[1].wait()
    inputs[2].wait()
    metas[me] = jnp.zeros(metas.shape[1:], F32)
    for e in range(n):
        metas[me, e:e + 1, :rows] = jnp.sum(
            jnp.where(idv[...] == e, rwv[...], 0.0), axis=0, keepdims=True)
    inputs[0].wait()
    pl.semaphore_wait(barrier, 3 + inner)
    for h in range(2):
        on_inner(lambda h=h: tok_copy(me, h, 1).start())
        tok_copy(me, h, 0).start()
    on_inner(lambda: meta_copy(me, 1).start())
    meta_copy(me, 0).start()
    for copy in weights:
        copy.start()

    @on_edge
    def _():
        cr[lax.rem(source[5] - me + n, n) - 1] = jnp.zeros((rows, width), BF16)

    def take(u):
        def wait():
            tok_copy(source[u], parity[u], 0).wait_recv()
            if u % 2:
                meta_copy(source[u], 0).wait_recv()

        on_edge(wait)

    def forward(u, away):
        def send():
            s, h = source[u], parity[u]
            tok_copy(s, h, 0).wait_recv()
            tok_copy(s, h, away).start()
            if u % 2:
                meta_copy(s, 0).wait_recv()
                meta_copy(s, away).start()

        on_inner(send)

    def project(*group):
        block = jnp.concatenate([toks[source[v], place(v)] for v in group], axis=0)
        for side, dst in ((1 - core, part), (core, own)):
            cols = pl.ds(pl.multiple_of(side * hh, hh), hh)
            for j, matrix in enumerate((gv.at[:, cols], uv.at[:, cols], turned.at[side])):
                result, first = dot(block, matrix[...]), 0
                for v in group:
                    dst[v, pl.ds(0, size[v]), pieces[j]] = result[first:first + size[v]]
                    first += size[v]
            if dst is part:
                for v in group:
                    mate_copy(v).start()

    def reduce(u):
        mine = pl.ds(0, size[u])
        mate_copy(u).wait_recv()
        total = own[u, mine] + peer[u, mine]
        own[u, mine] = total
        xs[u, mine] = total.astype(BF16)
        across_copy(u).start()

    def activate(u):
        mine = pl.ds(0, size[u])
        across_copy(u).wait_recv()
        gate, up, shared = [own[u, mine, cols] + xr[u, mine, cols].astype(F32) for cols in pieces]
        hid[u, core, mine, pl.ds(0, hh)] = (silu(gate) * up).astype(BF16)
        hid[u, core, mine, pl.ds(hh, ll)] = (silu(shared[:, :ll]) * shared[:, ll:]).astype(BF16)
        hid_copy(u).start()

    def finish(*group):
        scales = []
        for v in group:
            m = size[v]
            line = metas[source[v], pl.ds(me, 1), pl.ds(0, rows)]
            row = lax.broadcasted_iota(jnp.int32, (m, rows), 0) + parity[v] * half
            eye = row == lax.broadcasted_iota(jnp.int32, (m, rows), 1)
            scales.append(jnp.sum(jnp.where(eye, line, 0.0), axis=1, keepdims=True))
        scale = jnp.concatenate(scales, axis=0)
        for v in group:
            hid_copy(v).wait_recv()
        routed, shared = [
            jnp.concatenate([
                jnp.concatenate([hid[v, c, pl.ds(0, size[v]), cols] for c in range(2)], axis=1)
                for v in group], axis=0)
            for cols in (pl.ds(0, hh), pl.ds(hh, ll))
        ]
        def ship(c):
            for v in group:
                if v in (1, 2):
                    out_copy(v, c).start()
                elif v in (3, 4):
                    on_edge(lambda: out_copy(v, c).start())
                elif v:
                    on_edge(lambda: far_copy(v, c).start())
                    on_inner(lambda: out_copy(v, c).start())

        for c in range(width // chunk):
            cols = pl.ds(c * chunk, chunk)
            total, first = dot(routed, dv[:, cols]) * scale + dot(shared, sdv[:, cols]), 0
            for v in group:
                value = total[first:first + size[v]]
                first += size[v]
                if v == 0:
                    acc[:, cols] = value
                    continue
                cs[v - 1, :, cols] = value.astype(BF16)
                if v in (3, 4):
                    hold[v - 3, :, cols] = value
            if (c + 1) * chunk in (left, width):
                ship((c + 1) * chunk // width)

    def join(u, c):
        def add():
            far_copy(u + 2, c).wait_recv()
            cs[u - 1, :, sides[c]] = (
                hold[u - 3, :, sides[c]] + joint[u - 3, :, sides[c]].astype(F32)
            ).astype(BF16)
            out_copy(u, c).start()

        on_inner(add)

    for copy in weights[:2]:
        copy.wait()
    for side in range(2):
        for j, src in enumerate((sgv, suv)):
            turned[side, :, j * ll:(j + 1) * ll] = src[side * ll:(side + 1) * ll, :].T
    for copy in weights[2:4]:
        copy.wait()
    forward(1, 1)
    forward(5, 0)
    take(1)
    project(1, 0)
    reduce(1)
    forward(2, 1)
    forward(6, 0)
    take(2)
    project(2)
    reduce(2)
    forward(3, 1)
    take(3)
    project(3)
    activate(1)
    reduce(3)
    forward(4, 1)
    take(4)
    project(4)
    for copy in weights[4:]:
        copy.wait()
    finish(1)
    activate(2)
    reduce(4)
    take(5)
    project(5)
    finish(2)
    activate(3)
    reduce(5)
    take(6)
    project(6)
    finish(3)
    activate(4)
    reduce(6)
    reduce(0)
    finish(4)
    activate(5)
    finish(5)
    activate(6)
    finish(6)
    for u in (3, 4):
        for c in range(2):
            join(u, c)
    activate(0)
    finish(0)

    def landed(k):
        slot = lax.rem(source[k] - me + n, n) - 1
        for h in range(2):
            for c in range(2):
                remote(cs.at[0, :, sides[c]], cr.at[slot, span(h), sides[c]], c_ss.at[0, c],
                       c_rs.at[slot, h, c], {"ep": me + sign}).wait_recv()

    landed(1)
    landed(3)
    on_inner(lambda: landed(5))
    for u in range(len(size)):
        if u:
            for c in range(2):
                out_copy(u, c).wait_send()
        mate_copy(u).wait_send()
        across_copy(u).wait_send()
        hid_copy(u).wait_send()
    for h in range(2):
        tok_copy(me, h, 0).wait_send()
    meta_copy(me, 0).wait_send()

    @on_inner
    def _():
        meta_copy(me, 1).wait_send()
        for h in range(2):
            tok_copy(me, h, 1).wait_send()
        for u, away in ((1, 1), (2, 1), (3, 1), (4, 1), (5, 0), (6, 0)):
            tok_copy(source[u], parity[u], away).wait_send()
            if u % 2:
                meta_copy(source[u], away).wait_send()


def line_device(tokens, expert_ids, route_weights, gate_weight, up_weight, down_weight,
                shared_gate, shared_up, shared_down):
    n, ns = lax.axis_size("ep"), lax.axis_size("sub")
    rows, width = tokens.shape
    top = expert_ids.shape[1]
    hidden = gate_weight.shape[2]
    local = shared_gate.shape[0]
    both, units = hidden + local, 7
    dma = pltpu.SemaphoreType.DMA
    vmem = pl.BlockSpec(memory_space=pltpu.VMEM)
    hbm = pl.BlockSpec(memory_space=pl.ANY)
    total, sums = pl.pallas_call(
        functools.partial(line_kernel, n, ns, top),
        out_shape=(pltpu.VMEM((rows, width), F32), pltpu.VMEM((n - 1, rows, width), BF16)),
        in_specs=[hbm] * 9,
        out_specs=(vmem, vmem),
        scratch_shapes=[
            pltpu.VMEM((n, rows, width), BF16),
            pltpu.VMEM((n, -(-n // 8) * 8, -(-rows // 128) * 128), F32),
            pltpu.VMEM((top, rows), jnp.int32),
            pltpu.VMEM((top, rows), F32),
            pltpu.VMEM((width, hidden), BF16),
            pltpu.VMEM((width, hidden), BF16),
            pltpu.VMEM((hidden, width), BF16),
            pltpu.VMEM((local, width), BF16),
            pltpu.VMEM((local, width), BF16),
            pltpu.VMEM((local, width), BF16),
            pltpu.VMEM((2, width, local), BF16),
            pltpu.VMEM((units, rows, both), F32),
            pltpu.VMEM((units, rows, both), F32),
            pltpu.VMEM((units, rows, both), F32),
            pltpu.VMEM((units, rows, both), BF16),
            pltpu.VMEM((units, rows, both), BF16),
            pltpu.VMEM((units, 2, rows, both // 2), BF16),
            pltpu.VMEM((units - 1, rows // 2, width), BF16),
            pltpu.VMEM((2, rows // 2, width), F32),
            pltpu.VMEM((2, rows // 2, width), BF16),
            dma((6,)), dma((3,)),
            dma((n, 2, 2)), dma((n, 2)), dma((n, 2)), dma((n,)),
            dma((units,)), dma((units,)), dma((units,)), dma((units,)),
            dma((units,)), dma((units,)), dma((units - 1, 2)), dma((n - 1, 2, 2)), dma((2, 2)),
        ],
        compiler_params=pltpu.CompilerParams(collective_id=0, has_side_effects=True),
    )(tokens, expert_ids.T, route_weights.T, gate_weight, up_weight, down_weight,
      shared_gate, shared_up, shared_down)
    for slot in range(n - 1):
        total = total + sums[slot].astype(F32)
    return total.astype(BF16)


def solution(mesh):
    in_specs = (
        P(("groups", "ep"), "sub"),
        P(("groups", "ep"), None),
        P(("groups", "ep"), None),
        P("ep", "sub", None),
        P("ep", "sub", None),
        P("ep", None, "sub"),
        P("ep", "sub"),
        P("ep", "sub"),
        P("ep", "sub"),
    )
    out_specs = P(("groups", "ep"), "sub")
    line = mesh.shape["ep"] == 4 and mesh.shape["sub"] == 4
    return jax.shard_map(
        line_device if line else per_device, mesh=mesh, in_specs=in_specs, out_specs=out_specs, check_vma=False
    )
```
